16 devices in a mesh: dp: 2 (over z), tp: 8 (over x, y, core).
Axes of the slice: x: 2, y: 2, z: 2, core: 2. Of those that a mesh axis runs over, the one named last changes fastest.
Arguments:
- x: bfloat16 [2, 2048, 512], P('dp', 'tp')
- dy: bfloat16 [2, 2048, 512], P('dp', 'tp')
- wq: bfloat16 [512, 8192], P('dp', 'tp')
- wk: bfloat16 [512, 8192], P('dp', 'tp')
- wv: bfloat16 [512, 8192], P('dp', 'tp')
- wo: bfloat16 [8192, 512], P(('tp', 'dp'))
- w_gate: bfloat16 [512, 32768], P('dp', 'tp')
- w_up: bfloat16 [512, 32768], P('dp', 'tp')
- w_down: bfloat16 [32768, 512], P(('tp', 'dp'))
Outputs:
- output 1: bfloat16 [2, 2048, 512], P('dp', 'tp')
- output 2: bfloat16 [512, 8192], P('dp', 'tp')
- output 3: bfloat16 [512, 8192], P('dp', 'tp')
- output 4: bfloat16 [512, 8192], P('dp', 'tp')
- output 5: bfloat16 [8192, 512], P(('tp', 'dp'))
- output 6: bfloat16 [512, 32768], P('dp', 'tp')
- output 7: bfloat16 [512, 32768], P('dp', 'tp')
- output 8: bfloat16 [32768, 512], P(('tp', 'dp'))
All inputs are finite; a program needn't handle non-finite values.
Results may differ from the reference program's by a relative error of at most 0.024.
Values are sent between devices in bfloat16 or wider.
A program may use at most 2 GiB of HBM per device.

```python
import jax
import jax.numpy as jnp
from jax import lax

SEQUENCES = 2
TOKENS = 2048
D = 512
HEADS = 64
KV_HEADS = 64
HEAD = 128
FF = 32768
THETA = 10000
NAMES = ("wq", "wk", "wv", "wo", "w_gate", "w_up", "w_down")
SHAPES = {
    "wq": (D, HEADS * HEAD),
    "wk": (D, KV_HEADS * HEAD),
    "wv": (D, KV_HEADS * HEAD),
    "wo": (HEADS * HEAD, D),
    "w_gate": (D, FF),
    "w_up": (D, FF),
    "w_down": (FF, D),
}


def bump(key, n, height):
    away = (jnp.arange(n, dtype=jnp.int32) - jax.random.randint(key, (), 0, n, jnp.int32)) % n
    return jnp.where(away < n // 8, height, 1.0)


def together(key, own, strength):
    shared = jax.random.normal(key, own.shape[1:], jnp.float32)
    return (own + strength * shared) * lax.rsqrt(1 + strength * strength)


def setup_inputs(seed: int = 0, part: int = 0) -> dict:
    kx, kdy, ka, kb, kz, kf, kh, kl, *kw = jax.random.split(jax.random.key(seed), 8 + len(NAMES))
    shape = (SEQUENCES, TOKENS, D)
    much_x, much_dy = jax.random.uniform(kz, (2,), jnp.float32, 0.0, 1.0)
    loud = 2.0 ** jax.random.uniform(jax.random.fold_in(kz, 1), (), jnp.float32, -1.0, 2.0)
    halves = 2.0 ** jax.random.uniform(kl, (2,), jnp.float32, -1.0, 1.0)
    times = {"wq": 1.0, "wk": 1.0, "wv": 2.0, "wo": halves[0], "w_gate": 1.0, "w_up": bump(kh, FF, 4.0), "w_down": halves[1]}
    x = together(ka, jax.random.normal(kx, shape, jnp.float32), much_x) * bump(kf, D, 4.0)
    dy = together(kb, jax.random.normal(kdy, shape, jnp.float32), much_dy)
    drawn = {"x": x.astype(jnp.bfloat16), "dy": (loud * dy * (SEQUENCES * TOKENS) ** -0.5).astype(jnp.bfloat16)}
    for key, name in zip(kw, NAMES, strict=True):
        drawn[name] = (jax.random.normal(key, SHAPES[name], jnp.float32) * SHAPES[name][0] ** -0.5 * times[name]).astype(jnp.bfloat16)
    return drawn


def matmul(a, w):
    return jnp.dot(a, w, preferred_element_type=jnp.float32).astype(jnp.bfloat16)


def normed(h):
    wide = h.astype(jnp.float32)
    scale = lax.rsqrt(jnp.mean(wide**2, -1, keepdims=True) + 1e-6)
    return (wide * scale).astype(jnp.bfloat16)


def turned(t, theta):
    half = t.shape[-1] // 2
    angle = jnp.arange(t.shape[0], dtype=jnp.float32)[:, None] * theta ** (-jnp.arange(half, dtype=jnp.float32) / half)
    cos, sin = jnp.cos(angle)[:, None], jnp.sin(angle)[:, None]
    a, b = t[..., :half].astype(jnp.float32), t[..., half:].astype(jnp.float32)
    return jnp.concatenate([a * cos - b * sin, b * cos + a * sin], -1).astype(jnp.bfloat16)


def seen_by(q, k, v):
    tokens, kv = q.shape[0], k.shape[1]
    q = q.reshape(tokens, kv, -1, q.shape[-1])
    scores = jnp.einsum("tgsd,ugd->gstu", q.astype(jnp.float32), k.astype(jnp.float32)) * q.shape[-1] ** -0.5
    place = jnp.arange(tokens)
    weights = jax.nn.softmax(jnp.where(place[:, None] >= place, scores, -jnp.inf), -1).astype(jnp.bfloat16)
    return jnp.einsum("gstu,ugd->tgsd", weights.astype(jnp.float32), v.astype(jnp.float32)).astype(jnp.bfloat16).reshape(tokens, -1)


def layer(h, w):
    a = normed(h)
    q, k = (turned(matmul(a, w[name]).reshape(h.shape[0], -1, HEAD), THETA) for name in ("wq", "wk"))
    h = h + matmul(seen_by(q, k, matmul(a, w["wv"]).reshape(h.shape[0], -1, HEAD)), w["wo"])
    b = normed(h)
    gate = jnp.dot(b, w["w_gate"], preferred_element_type=jnp.float32)
    up = jnp.dot(b, w["w_up"], preferred_element_type=jnp.float32)
    return h + matmul((jax.nn.silu(gate) * up).astype(jnp.bfloat16), w["w_down"])


def reference(x, dy, wq, wk, wv, wo, w_gate, w_up, w_down):
    weights = dict(zip(NAMES, (wq, wk, wv, wo, w_gate, w_up, w_down), strict=True))

    def take(so_far, sequence):
        h, by_y = sequence
        _, back = jax.vjp(lambda w, h: layer(h, w), weights, h)
        by_weights, by_h = back(by_y)
        return jax.tree.map(lambda total, term: total + term.astype(jnp.float32), so_far, by_weights), by_h

    none_yet = {name: jnp.zeros(w.shape, jnp.float32) for name, w in weights.items()}
    by_weights, by_x = lax.scan(take, none_yet, (x, dy))
    return (by_x, *(by_weights[name].astype(jnp.bfloat16) for name in NAMES))
```

```python
import functools

import jax
import jax.numpy as jnp
import numpy as np
from jax import lax
from jax.experimental import pallas as pl
from jax.experimental.pallas import tpu as pltpu
from jax.sharding import PartitionSpec as P

NEG = -1e30
HIDDEN = 2 * NEG
LOG2E = 1.4426950408889634
VMEM = 60 * 2**20
HEAD = 128
THETA = 10000
EPS = 1e-6
F32, BF16 = jnp.float32, jnp.bfloat16


def _dot(a, b, ca, cb):
    return lax.dot_general(a, b, (((ca,), (cb,)), ((), ())), preferred_element_type=F32)


def nn(a, b):
    return _dot(a, b, 1, 0)


def nt(a, b):
    return _dot(a, b, 1, 1)


def tables(tokens):
    half = HEAD // 2
    angle = np.arange(tokens, dtype=np.float64)[:, None] * float(THETA) ** (-np.arange(half, dtype=np.float64) / half)
    cos, sin = np.cos(angle), np.sin(angle)
    return np.concatenate([cos, cos], -1).astype(np.float32), np.concatenate([-sin, sin], -1).astype(np.float32)


def normed(h):
    wide = h.astype(F32)
    scale = lax.rsqrt(jnp.mean(wide**2, -1, keepdims=True) + EPS)
    return (wide * scale).astype(BF16)


def norm_back(h, d):
    wide = h.astype(F32)
    scale = lax.rsqrt(jnp.mean(wide**2, -1, keepdims=True) + EPS)
    return scale * d - wide * (scale**3 * jnp.mean(d * wide, -1, keepdims=True))


MESH = pl.DeviceIdType.MESH
N_MSG = 17


def read(code):
    dz, flip, half = code
    return int(dz), int(flip), None if half == "-" else int(half)


def by(text, like):
    return [text[n : n + len(like)] for n in range(0, len(text), len(like))]


def kinds(text):
    return [(int(dz), int(flip)) for dz, flip in by(text, "--")]


def numbers(text):
    return [int(c, N_MSG) for c in text]


class Place:
    def __init__(self, piece):
        self.p, self.i = lax.axis_index("dp"), lax.axis_index("tp")
        self.piece = piece
        self.x, self.y, self.z, self.c = (self.p, self.i ^ 4), (self.p, self.i ^ 2), (1 - self.p, self.i), (self.p, self.i ^ 1)

    def rows(self, dz, flip, half=None):
        n = self.piece
        at = ((1 - self.p if dz else self.p) * 8 + (self.i ^ flip)) * n
        if half is None:
            return pl.ds(pl.multiple_of(at, n), n)
        return pl.ds(pl.multiple_of(at + half * (n // 2), n // 2), n // 2)

    def greet(self):
        barrier = pltpu.get_barrier_semaphore()
        for who in (self.x, self.y, self.z, self.c):
            pl.semaphore_signal(barrier, inc=1, device_id=who, device_id_type=MESH)
        pl.semaphore_wait(barrier, 4)


class Gather:
    COMES = [read(c) for c in by("10-04-02-01-14-12-11-06005-06103-16015-16113-07-17-", "---")]
    GOES = [(c[:1], *read(c[1:])) for c in by("z00-x00-y00-c00-x10-y10-c10-y040c04-x021c02-", "----") + by("y140c14-x121c12-c06-c16-", "----")]

    def __init__(self, place, all_ref, send, recv, first=0):
        self.place, self.all_ref, self.send, self.recv, self.first = place, all_ref, send, recv, first

    def copy(self, m, rows):
        src = self.all_ref.at[rows]
        return pltpu.make_async_remote_copy(src_ref=src, dst_ref=src, send_sem=self.send.at[self.first + m], recv_sem=self.recv.at[self.first + m],
                                            device_id=getattr(self.place, self.GOES[m][0]), device_id_type=MESH)

    def go(self, ms):
        for m in numbers(ms):
            self.copy(m, self.place.rows(*self.GOES[m][1:])).start()

    def come(self, ms):
        for m in numbers(ms):
            self.copy(m, self.place.rows(*self.COMES[m])).wait_recv()

    def start(self):
        self.go("1203")

    def middle(self):
        self.come("1")
        self.go("78")
        self.come("2")
        self.go("9a")
        self.come("0")
        self.go("456")

    def near(self):
        self.come("79")
        self.go("f")

    def late(self):
        self.come("4")
        self.go("bc")
        self.come("5")
        self.go("de")

    def last(self):
        self.come("bd")
        self.go("g")

    def sent(self):
        for m in range(N_MSG):
            self.copy(m, self.place.rows(*self.GOES[m][1:])).wait_send()


class Sum:
    KINDS = kinds("1614121006040200")

    def __init__(self, place, part_ref, peer, out, diag, block, across, send, recv, first=0):
        self.place, self.part_ref, self.peer, self.out, self.diag, self.block, self.across = place, part_ref, peer, out, diag, block, across
        self.send, self.recv, self.first = send, recv, first

    def copy(self, m, src, dst, who):
        return pltpu.make_async_remote_copy(src_ref=src, dst_ref=dst, send_sem=self.send.at[self.first + m], recv_sem=self.recv.at[self.first + m],
                                            device_id=who, device_id_type=MESH)

    def to_peer(self, k):
        dz, f = self.KINDS[k]
        return self.copy(k, self.part_ref.at[self.place.rows(dz, f ^ 1)], self.peer.at[k], self.place.c)

    def to_diag(self, dz, way):
        k, h = self.KINDS.index((dz, 6)), self.place.piece // 2
        return self.copy(8 + 2 * dz + way, self.out.at[k, pl.ds(way * h, h)], self.diag.at[dz, way], self.place.y if way else self.place.x)

    def to_block(self, dz, way):
        k = self.KINDS.index((dz, 2 if way else 4))
        return self.copy(12 + 2 * dz + way, self.out.at[k], self.block.at[dz, way], self.place.y if way else self.place.x)

    def to_z(self):
        return self.copy(16, self.out.at[self.KINDS.index((1, 0))], self.across, self.place.z)

    def both(self, k, half=None):
        dz, f = self.KINDS[k]
        self_rows = self.place.rows(dz, f, half)
        h = self.place.piece // 2
        mine = self.part_ref[self_rows, :].astype(F32)
        return mine + (self.peer[k] if half is None else self.peer[k, half * h : (half + 1) * h]).astype(F32)

    def start(self, dz, f):
        self.to_peer(self.KINDS.index((dz, f))).start()

    def deal(self, dz, f):
        k = self.KINDS.index((dz, f))
        h = self.place.piece // 2
        self.to_peer(k).wait_recv()
        if f == 6:
            self.out[k] = self.both(k).astype(BF16)
            self.to_diag(dz, 0).start()
            self.to_diag(dz, 1).start()
        elif f:
            way = 1 if f == 2 else 0
            self.to_diag(dz, 1 - way).wait_recv()
            joint = 1 - way
            self.out[k, joint * h : (joint + 1) * h] = (self.both(k, joint) + self.diag[dz, joint].astype(F32)).astype(BF16)
            self.out[k, way * h : (way + 1) * h] = self.both(k, way).astype(BF16)
            self.to_block(dz, way).start()
        else:
            self.to_block(dz, 0).wait_recv()
            self.to_block(dz, 1).wait_recv()
            total = self.both(k) + self.block[dz, 0].astype(F32) + self.block[dz, 1].astype(F32)
            if not dz:
                self.to_z().wait_recv()
                return total + self.across[...].astype(F32)
            self.out[k] = total.astype(BF16)
            self.to_z().start()

    def sent(self):
        for k in range(8):
            self.to_peer(k).wait_send()
        for dz in range(2):
            for way in range(2):
                self.to_diag(dz, way).wait_send()
                self.to_block(dz, way).wait_send()
        self.to_z().wait_send()


def sum_scratch(piece, d):
    return [pltpu.VMEM((8, piece, d), BF16), pltpu.VMEM((8, piece, d), BF16), pltpu.VMEM((2, 2, piece // 2, d), BF16),
            pltpu.VMEM((2, 2, piece, d), BF16), pltpu.VMEM((piece, d), BF16)]


def sems(n):
    return [pltpu.SemaphoreType.DMA((n,)), pltpu.SemaphoreType.DMA((n,))]


def comm_params(n):
    return pltpu.CompilerParams(collective_id=n, has_side_effects=True, vmem_limit_bytes=VMEM)


class Swap:
    def __init__(self, place, send, recv, first, what):
        self.place, self.send, self.recv, self.first, self.what = place, send, recv, first, what

    def copy(self, n):
        src, dst = self.what[n]
        return pltpu.make_async_remote_copy(src_ref=src, dst_ref=dst, send_sem=self.send.at[self.first + n], recv_sem=self.recv.at[self.first + n],
                                            device_id=self.place.z, device_id_type=MESH)

    def go(self, ns):
        for n in numbers(ns):
            self.copy(n).start()

    def come(self, ns):
        for n in numbers(ns):
            self.copy(n).wait_recv()

    def sent(self):
        for n in range(len(self.what)):
            self.copy(n).wait_send()


def pick(t, values):
    out = values[0]
    for n, v in enumerate(values):
        out = jnp.where(t == n, v, out)
    return out


def turn_of(kinds):
    p, i = lax.axis_index("dp"), lax.axis_index("tp")
    return lambda t: (pick(t, [1 - p if dz else p for dz, _ in kinds]), pick(t, [(i // 2) ^ (f // 2) for _, f in kinds]))


def whole(*shape):
    return pl.BlockSpec(shape, lambda *t: (0,) * len(shape), pipeline_mode=pl.Buffered(1))


def happen(t, at, events):
    for when, fn in events.items():
        step, place = when
        if place == at:
            pl.when(t == int(step))(fn)


def serial(*fns):
    def go():
        for fn in fns:
            fn()

    return go


def come(g, ms):
    return lambda: g.come(ms)


def calls(fn, *args):
    def go():
        for arg in args:
            fn(*arg)

    return go


ANY = pl.BlockSpec(memory_space=pl.ANY)
CHUNK = 512


def chunks(src, dst, to, at, cols):
    return [(src.at[:, pl.ds(pl.multiple_of(to + c, CHUNK), CHUNK)], dst.at[:, pl.ds(pl.multiple_of(at + c, CHUNK), CHUNK)]) for c in range(0, cols, CHUNK)]


FIRST = kinds("0010020406141216")


def _qkv(own_ref, wq_ref, wk_ref, wv_ref, wg_ref, cos_ref, sin_ref, out_ref, a_ref, wout_ref, got_ref, x_s, a_s, w_ref, send, recv, local):
    t = pl.program_id(0)
    m, n = lax.div(t, 8), lax.rem(t, 8)
    place = Place(own_ref.shape[0])
    both, half, cols, wide = 2 * place.piece, wq_ref.shape[0], w_ref.shape[2], wg_ref.shape[1] // 2
    g = Gather(place, x_s, send, recv)
    mine = pl.ds(pl.multiple_of(place.p * half, half), half)
    there = [(w.at[:, pl.ds(pl.multiple_of((1 - place.p) * cols, cols), cols)], w_ref.at[k, mine]) for k, w in enumerate((wq_ref, wk_ref, wv_ref))]
    there += chunks(wg_ref, got_ref, (1 - place.p) * wide, 0, CHUNK)
    z = Swap(place, send, recv, N_MSG, there)
    here = [pltpu.make_async_copy(w.at[:, pl.ds(pl.multiple_of(place.p * cols, cols), cols)], w_ref.at[k, mine], local.at[k])
            for k, w in enumerate((wq_ref, wk_ref, wv_ref))]

    def begin():
        for copy in here:
            copy.start()
        place.greet()
        x_s[place.rows(0, 0), :] = own_ref[...]
        g.start()
        z.go("0123")
        g.middle()
        g.near()
        for copy in here:
            copy.wait()
        z.come("0")
        g.come("3")

    happen(n + 8 * m, "-", {"0-": begin, "1-": come(g, "6"), "2-": come(g, "a"), "3-": come(g, "8"), "4-": come(g, "f"), "5-": serial(g.late, come(g, "c")),
                            "6-": come(g, "e"), "7-": serial(g.last, come(g, "g")), "8-": come(z, "1")})
    pl.when(t == 16)(come(z, "2"))
    seq, chip = turn_of(FIRST)(n)
    rows = pl.ds(pl.multiple_of((seq * 4 + chip) * both, both), both)

    @pl.when(m == 0)
    def _():
        a_s[rows, :] = normed(x_s[rows, :])
        a_ref[...] = a_s[rows, :]

    out = nn(a_s[rows, :], w_ref[m]).astype(BF16)

    @pl.when(m < 2)
    def _():
        cos, sin = cos_ref[...], sin_ref[...]
        for at in range(0, cols, HEAD):
            one = out[:, at : at + HEAD].astype(F32)
            out_ref[0, 0, :, at : at + HEAD] = (one * cos + pltpu.roll(one, HEAD // 2, 1) * sin).astype(BF16)

    @pl.when(m == 2)
    def _():
        out_ref[0, 0] = out

    @pl.when(t == pl.num_programs(0) - 1)
    def _():
        wout_ref[...] = w_ref[...]
        z.come("3")
        g.sent()
        z.sent()


def qkv(own, wq, wk, wv, wg, cos, sin, n):
    piece, d = own.shape
    both, cols, half = 2 * piece, wq.shape[1] // 2, wq.shape[0]
    at = lambda t: turn_of(FIRST)(lax.rem(t, 8))
    once = lambda t: at(jnp.minimum(t, 7))
    return pl.pallas_call(
        _qkv,
        grid=(24,),
        in_specs=[whole(piece, d)] + [ANY] * 4 + [pl.BlockSpec((both, HEAD), lambda t: (at(t)[1], 0))] * 2,
        out_specs=[pl.BlockSpec((1, 1, both, cols), lambda t: (lax.div(t, 8), *at(t), 0)), pl.BlockSpec((both, d), lambda t: (once(t)[0] * 4 + once(t)[1], 0)),
                   whole(3, d, cols), ANY],
        out_shape=[jax.ShapeDtypeStruct((3, 2, 8 * piece, cols), BF16), jax.ShapeDtypeStruct((16 * piece, d), BF16),
                   jax.ShapeDtypeStruct((3, d, cols), BF16), jax.ShapeDtypeStruct((half, CHUNK), BF16)],
        scratch_shapes=[pltpu.VMEM((16 * piece, d), BF16)] * 2 + [pltpu.VMEM((3, d, cols), BF16)] + sems(N_MSG + 4) + [pltpu.SemaphoreType.DMA((3,))],
        compiler_params=comm_params(n), name="qkv",
        cost_estimate=pl.CostEstimate(flops=96 * piece * d * cols, transcendentals=0, bytes_accessed=128 * piece * cols),
    )(own, wq, wk, wv, wg, cos, sin)


def _attend(q_ref, k_ref, v_ref, wo_ref, x_ref, dyo_ref, wg_ref, wu_ref, o_ref, lse_ref, h_ref, b_ref, dy_ref, gotg_ref, gotu_ref,
            top_s, mix_s, term_s, peer, out, diag, block_s, across, send, recv, local, *, scale, bk):
    t = pl.program_id(0)
    place = Place(x_ref.shape[0])
    heads, bq, wide = q_ref.shape[3] // HEAD, q_ref.shape[2], wg_ref.shape[1] // 2
    seq, iq = turn_of(Sum.KINDS)(t)
    e = scale * LOG2E
    g = Gather(place, dy_ref, send, recv)
    s = Sum(place, term_s, peer, out, diag, block_s, across, send, recv, N_MSG)
    other = (1 - place.p) * wide
    there = chunks(wg_ref, gotg_ref, other + CHUNK, 0, wide - CHUNK) + chunks(wu_ref, gotu_ref, other, 0, wide)
    z = Swap(place, send, recv, 2 * N_MSG, there)

    def begin():
        place.greet()
        copy = pltpu.make_async_copy(dyo_ref, dy_ref.at[place.rows(0, 0)], local.at[0])
        copy.start()
        copy.wait()
        g.start()
        z.go("0")

    def deal(n):
        return calls(s.deal, Sum.KINDS[n])

    def on(n):
        return lambda: z.go(n)

    events = {"0-": begin, "1-": on("1"), "2-": serial(on("2"), g.middle), "3-": serial(on("3"), g.near), "4-": serial(on("4"), g.late),
              "5-": serial(on("5"), g.last), "6-": on("6")}
    events |= {str(n + 1) + "+": deal(n) for n in range(7)}
    happen(t, "-", events)

    pieces = [slice(n * HEAD, (n + 1) * HEAD) for n in range(heads)]
    top_s[...] = jnp.full(top_s.shape, NEG, F32)
    mix_s[...] = jnp.zeros(mix_s.shape, F32)
    ones = jnp.ones((8, bk), BF16)

    def block(j, masked):
        here = pl.ds(pl.multiple_of(j * bk, bk), bk)
        scores = [nt(k_ref[0, 0, here, c], q_ref[0, 0, :, c]) for c in pieces]
        if masked:
            gap = lax.broadcasted_iota(jnp.int32, (bk, bq), 1) - lax.broadcasted_iota(jnp.int32, (bk, bq), 0)
            ok = gap >= j * bk - iq * bq
        weights, keeps = [], []
        for i, score in enumerate(scores):
            if masked:
                score = jnp.where(ok, score, HIDDEN)
            old = top_s[i : i + 1, :]
            top = jnp.maximum(old, score.max(axis=0, keepdims=True))
            top_s[i : i + 1, :] = top
            weights.append(jnp.exp2((score - top) * e).astype(BF16))
            keeps.append(jnp.exp2((old - top) * e))
        for i, (c, p, keep) in enumerate(zip(pieces, weights, keeps)):
            values = jnp.concatenate([v_ref[0, 0, here, c].T, ones], axis=0)
            mix_s[i] = mix_s[i] * keep + nn(values, p)

    full = lax.div(iq * bq, bk)
    lax.fori_loop(0, full, lambda j, _: block(j, False), None)
    happen(t, "+", events)
    lax.fori_loop(full, lax.div(iq * bq + bq + bk - 1, bk), lambda j, _: block(j, True), None)
    for i, c in enumerate(pieces):
        top, total = top_s[i : i + 1, :], mix_s[i, HEAD : HEAD + 1, :]
        o_ref[0, :, c] = (mix_s[i, :HEAD, :] * (1 / total)).T.astype(BF16)
        lse_ref[0, i : i + 1, :] = top * scale + jnp.log(total)
    term_s[pl.ds(pl.multiple_of((seq * 4 + iq) * bq, bq), bq), :] = nn(o_ref[0], wo_ref[...]).astype(BF16)
    for step, kind in enumerate(Sum.KINDS):
        pl.when(t == step)(functools.partial(s.start, *kind))

    @pl.when(t == pl.num_programs(0) - 1)
    def _():
        total = s.deal(*Sum.KINDS[-1])
        h = (x_ref[...].astype(F32) + total).astype(BF16)
        h_ref[...] = h
        b_ref[...] = normed(h)
        g.come("368acefg")
        z.come("0123456")
        g.sent()
        s.sent()
        z.sent()


def attend(qkvs, wo, x, dy, wg, wu, n, bk=512):
    _, seqs, tokens, cols = qkvs.shape
    piece, d = x.shape
    bq, heads, half, wide = 2 * piece, cols // HEAD, wg.shape[0], wg.shape[1] // 2
    at = lambda t: turn_of(Sum.KINDS)(t)
    return pl.pallas_call(
        functools.partial(_attend, scale=HEAD**-0.5, bk=bk),
        grid=(len(Sum.KINDS),),
        in_specs=[pl.BlockSpec((1, 1, bq, cols), lambda t: (0, *at(t), 0)), pl.BlockSpec((1, 1, tokens, cols), lambda t: (1, at(t)[0], 0, 0)),
                  pl.BlockSpec((1, 1, tokens, cols), lambda t: (2, at(t)[0], 0, 0)), whole(cols, d), whole(piece, d), whole(piece, d), ANY, ANY],
        out_specs=[pl.BlockSpec((1, bq, cols), lambda t: (*at(t), 0)), pl.BlockSpec((1, heads, bq), lambda t: (at(t)[0], 0, at(t)[1])),
                   whole(piece, d), whole(piece, d), ANY, ANY, ANY],
        out_shape=[jax.ShapeDtypeStruct((seqs, tokens, cols), BF16), jax.ShapeDtypeStruct((seqs, heads, tokens), F32)] +
                  [jax.ShapeDtypeStruct((piece, d), BF16)] * 2 + [jax.ShapeDtypeStruct((seqs * tokens, d), BF16),
                   jax.ShapeDtypeStruct((half, wide - CHUNK), BF16), jax.ShapeDtypeStruct((half, wide), BF16)],
        scratch_shapes=[pltpu.VMEM((8, bq), F32), pltpu.VMEM((heads, HEAD + 8, bq), F32), pltpu.VMEM((seqs * tokens, d), BF16)] + sum_scratch(piece, d) +
                       sems(2 * N_MSG + 7) + [pltpu.SemaphoreType.DMA((1,))],
        compiler_params=comm_params(n), name="attend",
        cost_estimate=pl.CostEstimate(flops=4 * seqs * tokens * tokens * cols, transcendentals=0, bytes_accessed=10 * seqs * tokens * cols),
    )(qkvs, qkvs, qkvs, wo, x, dy, wg, wu)


STEPS = kinds("0010061614120402")


def _units(own_ref, h_ref, dyo_ref, dy_ref, wd_ref, gate_ref, up_ref, got0_ref, got1_ref, got2_ref, dh_ref, gg_ref, gu_ref, gd_ref,
           wg_ref, wu_ref, b_s, db_s, g_s, u_s, d_s, peer, out, diag, block, across, send, recv, local, *, wide):
    t = pl.program_id(0)
    place = Place(own_ref.shape[0])
    both = 2 * place.piece
    g = Gather(place, b_s, send, recv)
    s = Sum(place, db_s, peer, out, diag, block, across, send, recv, N_MSG)

    half, ff = gate_ref.shape[0], wg_ref.shape[1]
    mine, theirs = (pl.ds(pl.multiple_of(p * half, half), half) for p in (place.p, 1 - place.p))
    cols = pl.ds(pl.multiple_of(place.p * ff, ff), ff)
    loads = [(gate_ref.at[:, cols], wg_ref.at[mine]), (up_ref.at[:, cols], wu_ref.at[mine]), (got2_ref, wu_ref.at[theirs]),
             (got0_ref, wg_ref.at[theirs, pl.ds(0, CHUNK)]), (got1_ref, wg_ref.at[theirs, pl.ds(CHUNK, ff - CHUNK)])]
    loads = [pltpu.make_async_copy(*pair, local.at[n]) for n, pair in enumerate(loads)]

    def begin():
        for copy in loads:
            copy.start()
        place.greet()
        b_s[place.rows(0, 0), :] = own_ref[...]
        g.start()
        for acc in (g_s, u_s, d_s):
            acc[...] = jnp.zeros_like(acc)
        for copy in loads:
            copy.wait()
        g.come("3")

    def deal(text):
        return calls(s.deal, *kinds(text))

    events = {"00": begin, "03": g.middle, "10": come(g, "6"), "11": g.near, "13": g.late, "20": come(g, "f"), "22": g.last, "30": come(g, "g"),
              "40": come(g, "c"), "50": come(g, "e"), "60": come(g, "8"), "70": come(g, "a")}
    events |= {"32": deal("06"), "42": deal("16"), "52": deal("14"), "62": deal("12"), "72": deal("0410")}
    seq, chip = turn_of(STEPS)(t)
    rows = pl.ds(pl.multiple_of((seq * 4 + chip) * both, both), both)
    db = bt = None
    for n, first in enumerate(range(0, wg_ref.shape[1], wide)):
        happen(t, str(n), events)
        if n == 0:
            b, dy = b_s[rows, :], dy_ref[rows, :]
            bt, dyt = b.T, dy.T
        here = slice(first, first + wide)
        gate, up = nn(b, wg_ref[:, here]), nn(b, wu_ref[:, here])
        dhid = nt(dy, wd_ref[here, :]).astype(BF16).astype(F32)
        sig = 1 / (1 + jnp.exp2(gate * -LOG2E))
        silu = gate * sig
        hid = (silu * up).astype(BF16)
        du = (dhid * silu).astype(BF16)
        dg = (dhid * up * (sig + silu * (1 - sig))).astype(BF16)
        term = nt(dg, wg_ref[:, here]) + nt(du, wu_ref[:, here])
        db = term if db is None else db + term
        g_s[:, here] += nn(bt, dg)
        u_s[:, here] += nn(bt, du)
        d_s[:, here] += nn(dyt, hid)
    db_s[rows, :] = db.astype(BF16)
    for step, kind in enumerate(STEPS):
        pl.when(t == step)(functools.partial(s.start, *kind))

    @pl.when(t == len(STEPS) - 1)
    def _():
        s.deal(0, 2)
        gg_ref[...] = g_s[...].astype(BF16)
        gu_ref[...] = u_s[...].astype(BF16)
        gd_ref[...] = d_s[...].T.astype(BF16)
        total = s.deal(0, 0)
        dh_ref[...] = (dyo_ref[...].astype(F32) + norm_back(h_ref[...], total)).astype(BF16)
        g.sent()
        s.sent()


def units(own, h, dyo, dy, wd, ws, n, wide=512):
    piece, d = own.shape
    tokens, ff = dy.shape[0], wd.shape[0]
    return pl.pallas_call(
        functools.partial(_units, wide=wide),
        grid=(len(STEPS),),
        in_specs=[whole(piece, d)] * 3 + [whole(tokens, d), whole(ff, d)] + [ANY] * 5,
        out_specs=[whole(piece, d), whole(d, ff), whole(d, ff), whole(ff, d)],
        out_shape=[jax.ShapeDtypeStruct((piece, d), BF16), jax.ShapeDtypeStruct((d, ff), BF16), jax.ShapeDtypeStruct((d, ff), BF16),
                   jax.ShapeDtypeStruct((ff, d), BF16)],
        scratch_shapes=[pltpu.VMEM((d, ff), BF16)] * 2 + [pltpu.VMEM((tokens, d), BF16)] * 2 + [pltpu.VMEM((d, ff), F32)] * 3 + sum_scratch(piece, d) + sems(2 * N_MSG) + [pltpu.SemaphoreType.DMA((5,))],
        compiler_params=comm_params(n),
        cost_estimate=pl.CostEstimate(flops=16 * tokens * d * ff, transcendentals=tokens * ff, bytes_accessed=6 * tokens * d + 12 * d * ff),
        name="units",
    )(own, h, dyo, dy, wd, *ws)


BACK = kinds("0002040610121416")


def _attend_back(q_ref, k_ref, v_ref, o_ref, own_ref, lse_ref, wo_ref, cos_ref, sin_ref, cosw_ref, sinw_ref, gg_ref, gu_ref,
                 dq_ref, dk_ref, dv_ref, go_ref, outg_ref, outu_ref, dh_s, do_s, dq_s, dk_s, dv_s, go_s, keep_s, send, recv, local, *, scale, bk):
    t = pl.program_id(0)
    place = Place(own_ref.shape[0])
    heads, bq, tokens, half, wide = q_ref.shape[3] // HEAD, q_ref.shape[2], k_ref.shape[2], outg_ref.shape[0], gg_ref.shape[1]
    seq, iq = turn_of(BACK)(t)
    e = scale * LOG2E
    g = Gather(place, dh_s, send, recv)
    theirs, mine = (pl.ds(pl.multiple_of(p * half, half), half) for p in (1 - place.p, place.p))
    there = chunks(gg_ref.at[theirs], outg_ref, 0, place.p * wide, wide) + chunks(gu_ref.at[theirs], outu_ref, 0, place.p * wide, wide)
    z = Swap(place, send, recv, N_MSG, there)
    cols = pl.ds(pl.multiple_of(place.p * wide, wide), wide)
    take = [pltpu.make_async_copy(a.at[mine], keep_s.at[n], local.at[n]) for n, a in enumerate((gg_ref, gu_ref))]
    put = [pltpu.make_async_copy(keep_s.at[n], a.at[:, cols], local.at[n]) for n, a in enumerate((outg_ref, outu_ref))]

    def begin():
        place.greet()
        dh_s[place.rows(0, 0), :] = own_ref[...]
        g.start()
        z.go("0")
        for copy in take:
            copy.start()
        go_s[...] = jnp.zeros_like(go_s)
        g.come("3")

    def first():
        g.middle()
        for a, b in zip(take, put):
            a.wait()
            b.start()
        g.come("a")

    def on(n):
        return lambda: z.go(n)

    happen(t, "-", {"0-": begin, "1-": serial(first, on("1")), "2-": serial(g.near, on("2"), come(g, "8")), "3-": serial(g.late, on("3"), come(g, "f")),
                    "4-": serial(g.last, on("4"), come(g, "6")), "5-": serial(on("5"), come(g, "e")), "6-": serial(on("6"), come(g, "c")),
                    "7-": serial(on("7"), come(g, "g"))})

    @pl.when(lax.rem(t, 4) == 0)
    def _():
        dk_s[...] = jnp.zeros_like(dk_s)
        dv_s[...] = jnp.zeros_like(dv_s)

    dh = dh_s[pl.ds(pl.multiple_of((seq * 4 + iq) * bq, bq), bq), :]
    dq_s[...] = jnp.zeros_like(dq_s)
    do_s[...] = nt(dh, wo_ref[...]).astype(BF16)
    go_s[...] += nn(o_ref[0].T, dh)
    parts = [slice(n * HEAD, (n + 1) * HEAD) for n in range(heads)]
    lses, deltas = [], []
    for n, c in enumerate(parts):
        lses.append(lse_ref[0, n : n + 1, :] * LOG2E)
        deltas.append((do_s[:, c].astype(F32) * o_ref[0, :, c].astype(F32)).T.sum(axis=0, keepdims=True))

    def block(j, masked):
        here = pl.ds(pl.multiple_of(j * bk, bk), bk)
        scores = [nt(k_ref[0, 0, here, c], q_ref[0, 0, :, c]) for c in parts]
        dps = [nt(v_ref[0, 0, here, c], do_s[:, c]) for c in parts]
        if masked:
            gap = lax.broadcasted_iota(jnp.int32, (bk, bq), 1) - lax.broadcasted_iota(jnp.int32, (bk, bq), 0)
            ok = gap >= j * bk - iq * bq
        for n, c in enumerate(parts):
            p = jnp.exp2(scores[n] * e - lses[n])
            if masked:
                p = jnp.where(ok, p, 0.0)
            ds = (p * (dps[n] - deltas[n])).astype(BF16)
            dv_s[n, here, :] += nn(p.astype(BF16), do_s[:, c])
            dk_s[n, here, :] += nn(ds, q_ref[0, 0, :, c])
            dq_s[n] += nn(k_ref[0, 0, here, c].T, ds)

    full = lax.div(iq * bq, bk)
    lax.fori_loop(0, full, lambda j, _: block(j, False), None)
    lax.fori_loop(full, lax.div(iq * bq + bq + bk - 1, bk), lambda j, _: block(j, True), None)

    def back(a, cos, sin):
        a = a * scale
        return (a * cos - pltpu.roll(a, HEAD // 2, 1) * sin).astype(BF16)

    for n, c in enumerate(parts):
        dq_ref[0, :, c] = back(dq_s[n].T, cos_ref[...], sin_ref[...])

    @pl.when(lax.rem(t, 4) == 3)
    def _():
        for n, c in enumerate(parts):
            dk_ref[0, :, c] = back(dk_s[n], cosw_ref[...], sinw_ref[...])
            dv_ref[0, :, c] = dv_s[n].astype(BF16)

    @pl.when(t == pl.num_programs(0) - 1)
    def _():
        go_ref[...] = go_s[...].astype(BF16)
        for copy in put:
            copy.wait()
        z.come("01234567")
        g.sent()
        z.sent()


def attend_back(qkvs, o, own, lse, wo, cos, sin, gg, gu, n, bk=512):
    _, seqs, tokens, cols = qkvs.shape
    piece, d = own.shape
    bq, heads, half, wide = 2 * piece, cols // HEAD, gg.shape[0] // 2, gg.shape[1]
    at = lambda t: turn_of(BACK)(t)
    block = pl.BlockSpec((1, bq, cols), lambda t: (*at(t), 0))
    every = pl.BlockSpec((1, tokens, cols), lambda t: (at(t)[0], 0, 0))
    table = pl.BlockSpec((bq, HEAD), lambda t: (at(t)[1], 0))
    return pl.pallas_call(
        functools.partial(_attend_back, scale=HEAD**-0.5, bk=bk),
        grid=(len(BACK),),
        in_specs=[pl.BlockSpec((1, 1, bq, cols), lambda t: (0, *at(t), 0)), pl.BlockSpec((1, 1, tokens, cols), lambda t: (1, at(t)[0], 0, 0)),
                  pl.BlockSpec((1, 1, tokens, cols), lambda t: (2, at(t)[0], 0, 0)), block, whole(piece, d),
                  pl.BlockSpec((1, heads, bq), lambda t: (at(t)[0], 0, at(t)[1])), whole(cols, d), table, table, whole(tokens, HEAD), whole(tokens, HEAD), ANY, ANY],
        out_specs=[block, every, every, whole(cols, d), ANY, ANY],
        out_shape=[jax.ShapeDtypeStruct((seqs, tokens, cols), BF16)] * 3 + [jax.ShapeDtypeStruct((cols, d), BF16)] +
                  [jax.ShapeDtypeStruct((half, 2 * wide), BF16)] * 2,
        scratch_shapes=[pltpu.VMEM((seqs * tokens, d), BF16), pltpu.VMEM((bq, cols), BF16), pltpu.VMEM((heads, HEAD, bq), F32), pltpu.VMEM((heads, tokens, HEAD), F32),
                        pltpu.VMEM((heads, tokens, HEAD), F32), pltpu.VMEM((cols, d), F32), pltpu.VMEM((2, half, wide), BF16)] + sems(N_MSG + 8) +
                       [pltpu.SemaphoreType.DMA((2,))],
        compiler_params=comm_params(n), name="attend_back",
        cost_estimate=pl.CostEstimate(flops=10 * seqs * tokens * tokens * cols, transcendentals=0, bytes_accessed=16 * seqs * tokens * cols),
    )(qkvs, qkvs, qkvs, o, own, lse, wo, cos, sin, cos, sin, gg, gu)


def _qkv_back(a_ref, dq_ref, dk_ref, dv_ref, w_ref, x_ref, dh_ref, dx_ref, gq_ref, gk_ref, gv_ref,
              sum_s, low_s, da_s, peer, out, diag, block, across, send, recv, local):
    t = pl.program_id(0)
    place = Place(x_ref.shape[0])
    both, half, cols = 2 * place.piece, gq_ref.shape[0], sum_s.shape[2]
    s = Sum(place, da_s, peer, out, diag, block, across, send, recv)
    theirs, mine = (pl.ds(pl.multiple_of(p * half, half), half) for p in (1 - place.p, place.p))
    at = pl.ds(pl.multiple_of(place.p * cols, cols), cols)
    outs = (gq_ref, gk_ref, gv_ref)
    z = Swap(place, send, recv, N_MSG, [(low_s.at[n, theirs], o.at[:, at]) for n, o in enumerate(outs)])
    keep = [pltpu.make_async_copy(low_s.at[n, mine], o.at[:, at], local.at[n]) for n, o in enumerate(outs)]
    grads = (dq_ref, dk_ref, dv_ref)

    @pl.when(t == 0)
    def _():
        place.greet()
        sum_s[...] = jnp.zeros_like(sum_s)

    @pl.when(t < 8)
    def _():
        across_a = a_ref[...].T
        for n, d in enumerate(grads):
            sum_s[n] += nn(across_a, d[0])

    @pl.when(t == 7)
    def _():
        low_s[...] = sum_s[...].astype(BF16)
        z.go("012")
        for copy in keep:
            copy.start()

    @pl.when(t >= 8)
    def _():
        seq, chip = turn_of(Sum.KINDS)(t - 8)
        da = [nt(d[0], w_ref[n]) for n, d in enumerate(grads)]
        da_s[pl.ds(pl.multiple_of((seq * 4 + chip) * both, both), both), :] = (da[0] + da[1] + da[2]).astype(BF16)

    for step, kind in enumerate(Sum.KINDS):
        pl.when(t == step + 8)(functools.partial(s.start, *kind))
        if step < 6:
            pl.when(t == step + 10)(calls(s.deal, kind))

    @pl.when(t == pl.num_programs(0) - 1)
    def _():
        s.deal(*Sum.KINDS[-2])
        total = s.deal(*Sum.KINDS[-1])
        dx_ref[...] = (dh_ref[...].astype(F32) + norm_back(x_ref[...], total)).astype(BF16)
        for copy in keep:
            copy.wait()
        z.come("012")
        z.sent()
        s.sent()


def qkv_back(a, dq, dk, dv, w, x, dh, n):
    piece, d = x.shape
    both, cols = 2 * piece, dq.shape[2]
    half = d // 2
    at = lambda t: tuple(jnp.where(t < 8, u, v) for u, v in zip((lax.div(t, 4), lax.rem(t, 4)), turn_of(Sum.KINDS)(t - 8)))
    grad = pl.BlockSpec((1, both, cols), lambda t: (*at(t), 0))
    return pl.pallas_call(
        _qkv_back,
        grid=(16,),
        in_specs=[pl.BlockSpec((both, d), lambda t: (jnp.minimum(t, 7), 0))] + [grad] * 3 + [whole(3, d, cols), whole(piece, d), whole(piece, d)],
        out_specs=[whole(piece, d)] + [ANY] * 3,
        out_shape=[jax.ShapeDtypeStruct((piece, d), BF16)] + [jax.ShapeDtypeStruct((half, 2 * cols), BF16)] * 3,
        scratch_shapes=[pltpu.VMEM((3, d, cols), F32), pltpu.VMEM((3, d, cols), BF16), pltpu.VMEM((16 * piece, d), BF16)] + sum_scratch(piece, d) +
                       sems(N_MSG + 3) + [pltpu.SemaphoreType.DMA((3,))],
        compiler_params=comm_params(n), name="qkv_back",
        cost_estimate=pl.CostEstimate(flops=192 * piece * d * cols, transcendentals=0, bytes_accessed=128 * piece * cols),
    )(a, dq, dk, dv, w, x, dh)


def solution(mesh):
    def step(x, dy, wq, wk, wv, wo, wg, wu, wd):
        x, dy = x[0], dy[0]
        cos, sin = (jnp.asarray(t) for t in tables(8 * x.shape[0]))
        qkvs, a, w, got0 = qkv(x, wq, wk, wv, wg, cos, sin, 0)
        o, lse, h, b, dys, got1, got2 = attend(qkvs, wo, x, dy, wg, wu, 1)
        dh, gg, gu, gd = units(b, h, dy, dys, wd, (wg, wu, got0, got1, got2), 2)
        dq, dk, dv, go, gg, gu = attend_back(qkvs, o, dh, lse, wo, cos, sin, gg, gu, 3)
        dx, gq, gk, gv = qkv_back(a, dq, dk, dv, w, x, dh, 4)
        return dx[None], gq, gk, gv, go, gg, gu, gd

    states, by_columns, by_rows = P("dp", "tp", None), P("dp", "tp"), P(("tp", "dp"), None)
    weights = (by_columns, by_columns, by_columns, by_rows, by_columns, by_columns, by_rows)
    return jax.shard_map(step, mesh=mesh, in_specs=(states, states, *weights), out_specs=(states, *weights), check_vma=False)
```

```python
import functools

import jax
import jax.numpy as jnp
import numpy as np
from jax import lax
from jax.experimental import pallas as pl
from jax.experimental.pallas import tpu as pltpu
from jax.sharding import PartitionSpec as P

NEG = -1e30
HIDDEN = 2 * NEG
LOG2E = 1.4426950408889634
VMEM = 60 * 2**20
HEAD = 128
THETA = 10000
EPS = 1e-6
F32, BF16 = jnp.float32, jnp.bfloat16


def _dot(a, b, ca, cb):
    return lax.dot_general(a, b, (((ca,), (cb,)), ((), ())), preferred_element_type=F32)


def nn(a, b):
    return _dot(a, b, 1, 0)


def nt(a, b):
    return _dot(a, b, 1, 1)


FINE = 32


def tables(tokens):
    half = HEAD // 2
    out = []
    for places in (np.arange(0, tokens, FINE), np.arange(FINE)):
        angle = places[:, None] * float(THETA) ** (-np.arange(half) / half)
        cos, sin = np.cos(angle), np.sin(angle)
        out += [np.concatenate(pair, -1).astype(np.float32) for pair in ((cos, cos), (-sin, sin))]
    return [jnp.asarray(t) for t in out]


def normed(h):
    wide = h.astype(F32)
    scale = lax.rsqrt(jnp.mean(wide**2, -1, keepdims=True) + EPS)
    return (wide * scale).astype(BF16)


def norm_back(h, d):
    wide = h.astype(F32)
    scale = lax.rsqrt(jnp.mean(wide**2, -1, keepdims=True) + EPS)
    return scale * d - wide * (scale**3 * jnp.mean(d * wide, -1, keepdims=True))


MESH = pl.DeviceIdType.MESH
N_MSG = 17


def read(code):
    dz, flip, half = code
    return int(dz), int(flip), None if half == "-" else int(half)


def by(text, like):
    return [text[n : n + len(like)] for n in range(0, len(text), len(like))]


def kinds(text):
    return [(int(dz), int(flip)) for dz, flip in by(text, "--")]


def numbers(text):
    return [int(c, N_MSG) for c in text]


class Place:
    def __init__(self, piece):
        self.p, self.i = lax.axis_index("dp"), lax.axis_index("tp")
        self.piece = piece
        self.x, self.y, self.z, self.c = (self.p, self.i ^ 4), (self.p, self.i ^ 2), (1 - self.p, self.i), (self.p, self.i ^ 1)

    def rows(self, dz, flip, half=None):
        n = self.piece
        at = ((1 - self.p if dz else self.p) * 8 + (self.i ^ flip)) * n
        if half is None:
            return pl.ds(pl.multiple_of(at, n), n)
        return pl.ds(pl.multiple_of(at + half * (n // 2), n // 2), n // 2)

    def greet(self):
        barrier = pltpu.get_barrier_semaphore()
        for who in (self.x, self.y, self.z, self.c):
            pl.semaphore_signal(barrier, inc=1, device_id=who, device_id_type=MESH)
        pl.semaphore_wait(barrier, 4)


class Gather:
    COMES = [read(c) for c in by("10-04-02-01-14-12-11-06005-06103-16015-16113-07-17-", "---")]
    GOES = [(c[:1], *read(c[1:])) for c in by("z00-x00-y00-c00-x10-y10-c10-y040c04-x021c02-", "----") + by("y140c14-x121c12-c06-c16-", "----")]

    def __init__(self, place, all_ref, send, recv, first=0):
        self.place, self.all_ref, self.send, self.recv, self.first = place, all_ref, send, recv, first

    def copy(self, m, rows):
        src = self.all_ref.at[rows]
        return pltpu.make_async_remote_copy(src_ref=src, dst_ref=src, send_sem=self.send.at[self.first + m], recv_sem=self.recv.at[self.first + m],
                                            device_id=getattr(self.place, self.GOES[m][0]), device_id_type=MESH)

    def go(self, ms):
        for m in numbers(ms):
            self.copy(m, self.place.rows(*self.GOES[m][1:])).start()

    def come(self, ms):
        for m in numbers(ms):
            self.copy(m, self.place.rows(*self.COMES[m])).wait_recv()

    def start(self):
        self.go("1203")

    def beside(self):
        self.come("1")
        self.go("78")
        self.come("2")
        self.go("9a")

    def beyond(self):
        self.come("0")
        self.go("456")

    def middle(self):
        self.beside()
        self.beyond()

    def near(self):
        self.come("79")
        self.go("f")

    def late(self):
        self.come("4")
        self.go("bc")
        self.come("5")
        self.go("de")

    def last(self):
        self.come("bd")
        self.go("g")

    def sent(self):
        for m in range(N_MSG):
            self.copy(m, self.place.rows(*self.GOES[m][1:])).wait_send()


class Sum:
    KINDS = kinds("1614121006040200")

    def __init__(self, place, part_ref, peer, out, diag, block, across, send, recv, first=0):
        self.place, self.part_ref, self.peer, self.out, self.diag, self.block, self.across = place, part_ref, peer, out, diag, block, across
        self.send, self.recv, self.first = send, recv, first

    def copy(self, m, src, dst, who):
        return pltpu.make_async_remote_copy(src_ref=src, dst_ref=dst, send_sem=self.send.at[self.first + m], recv_sem=self.recv.at[self.first + m],
                                            device_id=who, device_id_type=MESH)

    def to_peer(self, k):
        dz, f = self.KINDS[k]
        return self.copy(k, self.part_ref.at[self.place.rows(dz, f ^ 1)], self.peer.at[k], self.place.c)

    def to_diag(self, dz, way):
        k, h = self.KINDS.index((dz, 6)), self.place.piece // 2
        return self.copy(8 + 2 * dz + way, self.out.at[k, pl.ds(way * h, h)], self.diag.at[dz, way], self.place.y if way else self.place.x)

    def to_block(self, dz, way):
        k = self.KINDS.index((dz, 2 if way else 4))
        return self.copy(12 + 2 * dz + way, self.out.at[k], self.block.at[dz, way], self.place.y if way else self.place.x)

    def to_z(self):
        return self.copy(16, self.out.at[self.KINDS.index((1, 0))], self.across, self.place.z)

    def both(self, k, half=None):
        dz, f = self.KINDS[k]
        self_rows = self.place.rows(dz, f, half)
        h = self.place.piece // 2
        mine = self.part_ref[self_rows, :].astype(F32)
        return mine + (self.peer[k] if half is None else self.peer[k, half * h : (half + 1) * h]).astype(F32)

    def start(self, dz, f):
        self.to_peer(self.KINDS.index((dz, f))).start()

    def deal(self, dz, f):
        k = self.KINDS.index((dz, f))
        h = self.place.piece // 2
        self.to_peer(k).wait_recv()
        if f == 6:
            self.out[k] = self.both(k).astype(BF16)
            self.to_diag(dz, 0).start()
            self.to_diag(dz, 1).start()
        elif f:
            way = 1 if f == 2 else 0
            self.to_diag(dz, 1 - way).wait_recv()
            joint = 1 - way
            self.out[k, joint * h : (joint + 1) * h] = (self.both(k, joint) + self.diag[dz, joint].astype(F32)).astype(BF16)
            self.out[k, way * h : (way + 1) * h] = self.both(k, way).astype(BF16)
            self.to_block(dz, way).start()
        else:
            self.to_block(dz, 0).wait_recv()
            self.to_block(dz, 1).wait_recv()
            total = self.both(k) + self.block[dz, 0].astype(F32) + self.block[dz, 1].astype(F32)
            if not dz:
                self.to_z().wait_recv()
                return total + self.across[...].astype(F32)
            self.out[k] = total.astype(BF16)
            self.to_z().start()

    def sent(self):
        for k in range(8):
            self.to_peer(k).wait_send()
        for dz in range(2):
            for way in range(2):
                self.to_diag(dz, way).wait_send()
                self.to_block(dz, way).wait_send()
        self.to_z().wait_send()


def sum_scratch(piece, d):
    return [pltpu.VMEM((8, piece, d), BF16), pltpu.VMEM((8, piece, d), BF16), pltpu.VMEM((2, 2, piece // 2, d), BF16),
            pltpu.VMEM((2, 2, piece, d), BF16), pltpu.VMEM((piece, d), BF16)]


def sems(n):
    return [pltpu.SemaphoreType.DMA((n,)), pltpu.SemaphoreType.DMA((n,))]


def comm_params(n):
    return pltpu.CompilerParams(collective_id=n, has_side_effects=True, vmem_limit_bytes=VMEM)


def three(at, tokens, bq, cols):
    every = lambda which: pl.BlockSpec((None, None, tokens, cols), lambda t: (which, at(t)[0], 0, 0))
    return pl.BlockSpec((None, None, bq, cols), lambda t: (0, *at(t), 0)), every(1), every(2)


class Swap:
    def __init__(self, place, send, recv, first, what):
        self.place, self.send, self.recv, self.first, self.what = place, send, recv, first, what

    def copy(self, n):
        src, dst = self.what[n]
        return pltpu.make_async_remote_copy(src_ref=src, dst_ref=dst, send_sem=self.send.at[self.first + n], recv_sem=self.recv.at[self.first + n],
                                            device_id=self.place.z, device_id_type=MESH)

    def go(self, ns):
        for n in numbers(ns):
            self.copy(n).start()

    def come(self, ns):
        for n in numbers(ns):
            self.copy(n).wait_recv()

    def sent(self):
        for n in range(len(self.what)):
            self.copy(n).wait_send()


def bit(t, bits):
    return (np.int32(np.array(sum(b << n for n, b in enumerate(bits)), np.uint32).view(np.int32)) >> t) & 1


def pick(t, values):
    return bit(t, [v & 1 for v in values]) + 2 * bit(t, [v >> 1 for v in values])


def turn_of(kinds):
    p, i = lax.axis_index("dp"), lax.axis_index("tp")
    return lambda t: (p ^ bit(t, [dz for dz, _ in kinds]), (i // 2) ^ pick(t, [f // 2 for _, f in kinds]))


def whole(*shape):
    return pl.BlockSpec(shape, lambda *t: (0,) * len(shape), pipeline_mode=pl.Buffered(1))


def happen(t, at, events):
    for when, fn in events.items():
        if when[1:] in ("", at):
            pl.when(t == int(when[0]))(fn)


def serial(*fns):
    def go():
        for fn in fns:
            fn()

    return go


def come(g, ms):
    return lambda: g.come(ms)


def calls(fn, *args):
    def go():
        for arg in args:
            fn(*arg)

    return go


ANY, IN_VMEM = pl.BlockSpec(memory_space=pl.ANY), pl.BlockSpec(memory_space=pltpu.VMEM)
CHUNK = 512
EARLY = 2 * CHUNK


def chunks(src, dst, to, at, cols):
    return [(src.at[:, pl.ds(pl.multiple_of(to + c, CHUNK), CHUNK)], dst.at[:, pl.ds(pl.multiple_of(at + c, CHUNK), CHUNK)]) for c in range(0, cols, CHUNK)]


FIRST = kinds("0010020406141216")
HIDE = kinds("0002041006141216")


def _qkv(own_ref, dyo_ref, cos0_ref, sin0_ref, cos1_ref, sin1_ref, wdin_ref, wq_ref, wk_ref, wv_ref, wg_ref,
         out_ref, at_ref, wout_ref, got_ref, dy_ref, hide_ref, cosout_ref, sinout_ref,
         x_s, a_s, at_s, out_s, w_s, dy_s, hide_s, wd_ref, cos_ref, sin_ref, send, recv, local, loaded):
    place = Place(own_ref.shape[0])
    tokens, cols = cos_ref.shape[0], w_s.shape[2]
    both, half, wide = 2 * place.piece, wq_ref.shape[0], wg_ref.shape[1] // 2
    g = Gather(place, x_s, send, recv)
    mine = pl.ds(pl.multiple_of(place.p * half, half), half)
    weights = (wq_ref, wk_ref, wv_ref)
    there = [(w.at[:, pl.ds(pl.multiple_of((1 - place.p) * cols, cols), cols)], w_s.at[k, mine]) for k, w in enumerate(weights)]
    there += chunks(wg_ref, got_ref, (1 - place.p) * wide, 0, EARLY)
    z = Swap(place, send, recv, 2 * N_MSG, there)
    d = Gather(place, dy_s, send, recv, N_MSG)
    here = [pltpu.make_async_copy(w.at[:, pl.ds(pl.multiple_of(place.p * cols, cols), cols)], w_s.at[k, mine], local.at[k]) for k, w in enumerate(weights)]
    load = [pltpu.make_async_copy(*pair, loaded.at[k]) for k, pair in enumerate([(wdin_ref, wd_ref)])]
    for copy in load + here:
        copy.start()
    place.greet()
    x_s[place.rows(0, 0), :] = own_ref[...]
    dy_s[place.rows(0, 0), :] = dyo_ref[...]
    g.start()
    z.go("01")
    d.go("03")
    z.go("234")

    def turns(n, _):
        rows = pl.ds(pl.multiple_of(n * FINE, FINE), FINE)
        cos, sin = cos0_ref[pl.ds(n, 1), :], sin0_ref[pl.ds(n, 1), :]
        cos_ref[rows, :] = cos * cos1_ref[...] - sin * sin1_ref[...]
        sin_ref[rows, :] = sin * cos1_ref[...] + cos * sin1_ref[...]

    lax.fori_loop(0, tokens // FINE, turns, None)
    table_copies = [pltpu.make_async_copy(*pair, loaded.at[k + 1]) for k, pair in enumerate([(cos_ref, cosout_ref), (sin_ref, sinout_ref)])]
    for copy in table_copies:
        copy.start()

    def hide(rows):
        for c in range(0, hide_s.shape[1], CHUNK):
            hide_s[rows, c : c + CHUNK] = nt(dy_s[rows, :], wd_ref[c : c + CHUNK, :]).astype(BF16)
        pltpu.make_async_copy(hide_s.at[rows], hide_ref.at[rows], local.at[5]).start()
        pltpu.make_async_copy(dy_s.at[rows], dy_ref.at[rows], local.at[6]).start()

    def result(m, rows, a):
        t = nn(a, w_s[m]).astype(BF16)
        if m < 2:
            here = pl.ds(pl.multiple_of(lax.rem(rows.start, tokens), both), both)
            cos, sin = cos_ref[here, :], sin_ref[here, :]
            for at in range(0, cols, HEAD):
                one = t[:, at : at + HEAD].astype(F32)
                out_s[m, rows, at : at + HEAD] = (one * cos + pltpu.roll(one, HEAD // 2, 1) * sin).astype(BF16)
        else:
            out_s[m, rows, :] = t
        pltpu.make_async_copy(out_s.at[m, rows], out_ref.at[m, rows], local.at[m]).start()

    def first(rows):
        a = normed(x_s[rows, :])
        a_s[rows, :] = a
        at_s[:, rows] = a.T
        result(0, rows, a)

    def later(m):
        return lambda rows: result(m, rows, a_s[rows, :])

    at_copy = pltpu.make_async_copy(at_s, at_ref, local.at[3])
    w_copy = pltpu.make_async_copy(w_s, wout_ref, local.at[4])

    def loads():
        for copy in here:
            copy.wait()

    ways = {"h": (hide, HIDE, zip("1234567", "a86fceg"), d), "q": (first, FIRST, zip("1234567", "6a8fceg"), g), "k": (later(1), FIRST, (), None),
            "v": (later(2), FIRST, (), None)}
    ways = {name: (fn, order, list(needs), who) for name, (fn, order, needs, who) in ways.items()}

    def run(code):
        name, a, b = code
        fn, order, needs, who = ways[name]

        def one(n, _):
            for at, ms in needs:
                if a <= at < b:
                    pl.when(n == int(at))(come(who, ms))
            seq, chip = turn_of(order)(n)
            fn(pl.ds(pl.multiple_of((seq * 4 + chip) * both, both), both))

        lax.fori_loop(int(a), int(b), one, None)

    d.come("3")
    load[0].wait()
    run("h01")
    g.middle()
    d.go("12")
    g.near()
    loads()
    z.come("0")
    g.come("3")
    run("q05")
    g.late()
    run("q57")
    z.come("1")
    run("k07")
    d.beside()
    run("h13")
    g.last()
    run("q78")
    at_copy.start()
    run("k78")
    d.beyond()
    d.near()
    run("h35")
    z.come("2")
    w_copy.start()
    run("v08")
    d.late()
    run("h57")
    d.last()
    run("h78")
    at_copy.wait()
    w_copy.wait()
    for m in range(3):
        pltpu.make_async_copy(out_s.at[m], out_ref.at[m], local.at[m]).wait()
    z.come("34")
    g.sent()
    d.sent()
    z.sent()
    for copy in table_copies:
        copy.wait()
    pltpu.make_async_copy(hide_s, hide_ref, local.at[5]).wait()
    pltpu.make_async_copy(dy_s, dy_ref, local.at[6]).wait()


def qkv(own, dy, wd, wq, wk, wv, wg, tokens, n):
    piece, d = own.shape
    given, table = tables(tokens), (tokens, HEAD)
    tokens, cols, half = 16 * piece, wq.shape[1] // 2, wq.shape[0]
    shapes = [(3, tokens, cols), (d, tokens), (3, d, cols), (half, EARLY), (tokens, d), (tokens, wd.shape[0])]
    return pl.pallas_call(
        _qkv,
        in_specs=[IN_VMEM] * 6 + [ANY] * 5,
        out_specs=[ANY] * 8,
        out_shape=[jax.ShapeDtypeStruct(shape, BF16) for shape in shapes] + [jax.ShapeDtypeStruct(table, F32)] * 2,
        scratch_shapes=[pltpu.VMEM(shape, BF16) for shape in [(tokens, d)] * 2 + [(d, tokens), (3, tokens, cols), (3, d, cols), *shapes[4:], wd.shape]] +
                       [pltpu.VMEM(table, F32)] * 2 + sems(2 * N_MSG + 5) + [pltpu.SemaphoreType.DMA((7,)), pltpu.SemaphoreType.DMA((3,))],
        compiler_params=comm_params(n), name="qkv",
        cost_estimate=pl.CostEstimate(flops=6 * tokens * d * cols, transcendentals=0, bytes_accessed=8 * tokens * cols),
    )(own, dy, *given, wd, wq, wk, wv, wg)


def _attend(q_ref, k_ref, v_ref, wo_ref, x_ref, wg_ref, wu_ref, o_ref, lse_ref, h_ref, b_ref, gotg_ref, gotu_ref,
            top_s, mix_s, term_s, peer, out, diag, block_s, across, send, recv, *, scale, bk):
    t = pl.program_id(0)
    place = Place(x_ref.shape[0])
    bq, width = q_ref.shape
    heads, wide = width // HEAD, wg_ref.shape[1] // 2
    seq, iq = turn_of(Sum.KINDS)(t)
    e = scale * LOG2E
    s = Sum(place, term_s, peer, out, diag, block_s, across, send, recv)
    other = (1 - place.p) * wide
    there = chunks(wg_ref, gotg_ref, other + EARLY, 0, wide - EARLY) + chunks(wu_ref, gotu_ref, other, 0, wide - CHUNK)
    z = Swap(place, send, recv, N_MSG, there)

    def begin():
        place.greet()
        z.go("01")

    def deal(n):
        return calls(s.deal, Sum.KINDS[n])

    def on(n):
        return lambda: z.go(n)

    events = {"0-": begin, "1-": on("2"), "2-": on("3"), "5-": on("4")}
    events |= {when: deal(n) for n, when in enumerate(by("1+2+3+6-5+6+7+", "--"))}
    happen(t, "-", events)

    pieces = [slice(n * HEAD, (n + 1) * HEAD) for n in range(heads)]
    top_s[...] = jnp.full(top_s.shape, NEG, F32)
    mix_s[...] = jnp.zeros(mix_s.shape, F32)
    def tile(first, keys, q0, masked):
        here = pl.ds(pl.multiple_of(first, keys), keys)
        scores = [nt(k_ref[here, c], q_ref[q0:, c]) for c in pieces]
        if masked:
            shape = (keys, bq - q0)
            ok = lax.broadcasted_iota(jnp.int32, shape, 1) >= lax.broadcasted_iota(jnp.int32, shape, 0)
        weights, keeps = [], []
        for i, score in enumerate(scores):
            if masked:
                score = jnp.where(ok, score, HIDDEN)
            old = top_s[i : i + 1, q0:]
            top = jnp.maximum(old, score.max(axis=0, keepdims=True))
            top_s[i : i + 1, q0:] = top
            weights.append(jnp.exp2((score - top) * e).astype(BF16))
            keeps.append(jnp.exp2((old - top) * e))
        ones = jnp.ones((8, keys), BF16)
        for i, (c, p, keep) in enumerate(zip(pieces, weights, keeps)):
            values = jnp.concatenate([v_ref[here, c].T, ones], axis=0)
            mix_s[i, :, q0:] = mix_s[i, :, q0:] * keep + nn(values, p)

    lax.fori_loop(0, iq, lambda j, _: tile(j * bq, bq, 0, False), None)
    happen(t, "+", events)
    for q0 in range(0, bq, bk):
        tile(iq * bq + q0, bk, q0, True)
    for i, c in enumerate(pieces):
        top, total = top_s[i : i + 1, :], mix_s[i, HEAD : HEAD + 1, :]
        o_ref[:, c] = (mix_s[i, :HEAD, :] * (1 / total)).T.astype(BF16)
        lse_ref[i : i + 1, :] = top * scale + jnp.log(total)
    term_s[pl.ds(pl.multiple_of((seq * 4 + iq) * bq, bq), bq), :] = nn(o_ref[...], wo_ref[...]).astype(BF16)
    for step, kind in enumerate(Sum.KINDS):
        pl.when(t == step)(functools.partial(s.start, *kind))

    @pl.when(t == pl.num_programs(0) - 1)
    def _():
        total = s.deal(*Sum.KINDS[-1])
        h = (x_ref[...].astype(F32) + total).astype(BF16)
        h_ref[...] = h
        b_ref[...] = normed(h)
        z.come("01234")
        s.sent()
        z.sent()


def attend(qkvs, wo, x, wg, wu, n, bk=256):
    _, seqs, tokens, cols = qkvs.shape
    piece, d = x.shape
    bq, heads, half, wide = 2 * piece, cols // HEAD, wg.shape[0], wg.shape[1] // 2
    at = lambda t: turn_of(Sum.KINDS)(t)
    return pl.pallas_call(
        functools.partial(_attend, scale=HEAD**-0.5, bk=bk),
        grid=(len(Sum.KINDS),),
        in_specs=[*three(at, tokens, bq, cols), whole(cols, d), whole(piece, d), ANY, ANY],
        out_specs=[pl.BlockSpec((None, bq, cols), lambda t: (*at(t), 0)), pl.BlockSpec((None, heads, bq), lambda t: (at(t)[0], 0, at(t)[1])),
                   whole(piece, d), whole(piece, d), ANY, ANY],
        out_shape=[jax.ShapeDtypeStruct((seqs, tokens, cols), BF16), jax.ShapeDtypeStruct((seqs, heads, tokens), F32)] +
                  [jax.ShapeDtypeStruct((piece, d), BF16)] * 2 + [jax.ShapeDtypeStruct((half, wide - EARLY), BF16), jax.ShapeDtypeStruct((half, wide - CHUNK), BF16)],
        scratch_shapes=[pltpu.VMEM((8, bq), F32), pltpu.VMEM((heads, HEAD + 8, bq), F32), pltpu.VMEM((seqs * tokens, d), BF16)] + sum_scratch(piece, d) +
                       sems(N_MSG + 5),
        compiler_params=comm_params(n), name="attend",
        cost_estimate=pl.CostEstimate(flops=4 * seqs * tokens * tokens * cols, transcendentals=0, bytes_accessed=10 * seqs * tokens * cols),
    )(qkvs, qkvs, qkvs, wo, x, wg, wu)


STEPS = kinds("0004101614120602")


def _units(own_ref, h_ref, dyo_ref, dy_ref, hide_ref, gate_ref, up_ref, got0_ref, got1_ref, got2_ref, dh_ref, gg_ref, gu_ref, gd_ref,
           wg_ref, wu_ref, b_s, db_s, g_s, u_s, d_s, low_s, last_s, bt_s, dyt_s, sum_s, peer, out, diag, block, across, send, recv, local, *, wide):
    t = pl.program_id(0)
    place = Place(own_ref.shape[0])
    both = 2 * place.piece
    g = Gather(place, b_s, send, recv)
    s = Sum(place, db_s, peer, out, diag, block, across, send, recv, N_MSG)

    half, ff = gate_ref.shape[0], wg_ref.shape[1]
    mine, theirs = (pl.ds(pl.multiple_of(p * half, half), half) for p in (place.p, 1 - place.p))
    cols = pl.ds(pl.multiple_of(place.p * ff, ff), ff)
    loads = [(gate_ref.at[:, cols], wg_ref.at[mine]), (up_ref.at[:, cols], wu_ref.at[mine]), (got2_ref, wu_ref.at[theirs, pl.ds(0, ff - CHUNK)]),
             (got0_ref, wg_ref.at[theirs, pl.ds(0, EARLY)]), (got1_ref, wg_ref.at[theirs, pl.ds(EARLY, ff - EARLY)])]
    other = pl.ds(pl.multiple_of((2 - place.p) * ff - CHUNK, CHUNK), CHUNK)
    z = Swap(place, send, recv, 2 * N_MSG, [(up_ref.at[:, other], wu_ref.at[mine, pl.ds(ff - CHUNK, CHUNK)])])
    loads = [pltpu.make_async_copy(*pair, local.at[n]) for n, pair in enumerate(loads)]

    def begin():
        for copy in loads:
            copy.start()
        place.greet()
        b_s[place.rows(0, 0), :] = own_ref[...]
        z.go("0")
        g.start()
        for acc in (g_s, u_s, d_s):
            acc[...] = jnp.zeros_like(acc)
        for copy in loads:
            copy.wait()
        g.come("3")

    def deal(text):
        return calls(s.deal, *kinds(text))

    def beside():
        g.beside()
        z.come("0")

    def beyond():
        g.near()
        g.beyond()

    events = {"00": begin, "03": beside, "10": come(g, "8"), "12": beyond, "20": come(g, "6"), "21": g.late, "23": g.last, "30": come(g, "g"),
              "40": come(g, "c"), "50": come(g, "e"), "60": come(g, "f"), "70": come(g, "a")}
    events |= {"42": deal("16"), "52": deal("14"), "62": deal("12"), "72": deal("0610")}
    seq, chip = turn_of(STEPS)(t)
    rows = pl.ds(pl.multiple_of((seq * 4 + chip) * both, both), both)
    happen(t, "0", events)
    bt_s[...] = b_s[rows, :].T
    dyt_s[...] = dy_ref[...].T
    sum_s[...] = jnp.zeros_like(sum_s)

    def pair(m, _):
        for w in range(2):
            for when, fn in events.items():
                step, n = int(when[0]), int(when[1])
                if n and n % 2 == w:
                    pl.when((t == step) & (m == n // 2))(fn)
            here = pl.ds(pl.multiple_of((2 * m + w) * wide, wide), wide)
            b = b_s[rows, :]
            gate, up = nn(b, wg_ref[:, here]), nn(b, wu_ref[:, here])
            dhid = hide_ref[:, here].astype(F32)
            sig = 1 / (1 + jnp.exp2(gate * -LOG2E))
            silu = gate * sig
            hid = (silu * up).astype(BF16)
            du = (dhid * silu).astype(BF16)
            dg = (dhid * up * (sig + silu * (1 - sig))).astype(BF16)
            sum_s[...] += nt(dg, wg_ref[:, here]) + nt(du, wu_ref[:, here])
            g_s[:, here] += nn(bt_s[...], dg)
            u_s[:, here] += nn(bt_s[...], du)
            d_s[:, here] += nn(dyt_s[...], hid)

    lax.fori_loop(0, wg_ref.shape[1] // (2 * wide), pair, None)
    db = sum_s[...]
    db_s[rows, :] = db.astype(BF16)
    for step, kind in enumerate(STEPS):
        pl.when(t == step)(functools.partial(s.start, *kind))

    @pl.when(t == len(STEPS) - 1)
    def _():
        s.deal(0, 2)
        s.deal(0, 4)
        low_s[0] = g_s[...].astype(BF16)
        low_s[1] = u_s[...].astype(BF16)
        last_s[...] = d_s[...].T.astype(BF16)
        saves = [pltpu.make_async_copy(*pair, local.at[k]) for k, pair in enumerate([(low_s.at[0], gg_ref), (low_s.at[1], gu_ref), (last_s, gd_ref)])]
        for copy in saves:
            copy.start()
        total = s.deal(0, 0)
        dh_ref[...] = (dyo_ref[...].astype(F32) + norm_back(h_ref[...], total)).astype(BF16)
        g.sent()
        s.sent()
        z.sent()
        for copy in saves:
            copy.wait()


def units(own, h, dyo, dy, hide, ws, n, wide=512):
    piece, d = own.shape
    tokens, ff = hide.shape
    at = lambda t: turn_of(STEPS)(t)
    return pl.pallas_call(
        functools.partial(_units, wide=wide),
        grid=(len(STEPS),),
        in_specs=[whole(piece, d)] * 3 + [pl.BlockSpec((2 * piece, width), lambda t: (at(t)[0] * 4 + at(t)[1], 0)) for width in (d, ff)] + [ANY] * 5,
        out_specs=[whole(piece, d)] + [ANY] * 3,
        out_shape=[jax.ShapeDtypeStruct((piece, d), BF16), jax.ShapeDtypeStruct((d, ff), BF16), jax.ShapeDtypeStruct((d, ff), BF16),
                   jax.ShapeDtypeStruct((ff, d), BF16)],
        scratch_shapes=[pltpu.VMEM((d, ff), BF16)] * 2 + [pltpu.VMEM((tokens, d), BF16)] * 2 + [pltpu.VMEM((d, ff), F32)] * 3 + [pltpu.VMEM((2, d, ff), BF16), pltpu.VMEM((ff, d), BF16)] +
                       [pltpu.VMEM((d, 2 * piece), BF16)] * 2 + [pltpu.VMEM((2 * piece, d), F32)] + sum_scratch(piece, d) + sems(2 * N_MSG + 1) + [pltpu.SemaphoreType.DMA((5,))],
        compiler_params=comm_params(n),
        cost_estimate=pl.CostEstimate(flops=16 * tokens * d * ff, transcendentals=tokens * ff, bytes_accessed=6 * tokens * d + 12 * d * ff),
        name="units",
    )(own, h, dyo, dy, hide, *ws)


BACK = kinds("0002040610121416")


def _attend_back(q_ref, k_ref, v_ref, o_ref, own_ref, lse_ref, wo_ref, cos_ref, sin_ref, cosw_ref, sinw_ref, gg_ref, gu_ref,
                 dq_ref, dk_ref, dv_ref, go_ref, outg_ref, outu_ref, dh_s, do_s, dq_s, dk_s, dv_s, go_s, keep_s, send, recv, local, *, scale, bk):
    t = pl.program_id(0)
    place = Place(own_ref.shape[0])
    bq, width = q_ref.shape
    heads, half, wide = width // HEAD, outg_ref.shape[0], gg_ref.shape[1]
    seq, iq = turn_of(BACK)(t)
    e = scale * LOG2E
    g = Gather(place, dh_s, send, recv)
    theirs, mine = (pl.ds(pl.multiple_of(p * half, half), half) for p in (1 - place.p, place.p))
    there = chunks(gg_ref.at[theirs], outg_ref, 0, place.p * wide, wide) + chunks(gu_ref.at[theirs], outu_ref, 0, place.p * wide, wide)
    z = Swap(place, send, recv, N_MSG, there)
    cols = pl.ds(pl.multiple_of(place.p * wide, wide), wide)
    take = [pltpu.make_async_copy(a.at[mine], keep_s.at[n], local.at[n]) for n, a in enumerate((gg_ref, gu_ref))]
    put = [pltpu.make_async_copy(keep_s.at[n], a.at[:, cols], local.at[n]) for n, a in enumerate((outg_ref, outu_ref))]

    def begin():
        place.greet()
        dh_s[place.rows(0, 0), :] = own_ref[...]
        g.start()
        z.go("0")
        for copy in take:
            copy.start()
        go_s[...] = jnp.zeros_like(go_s)
        g.come("3")

    def first():
        g.middle()
        for a, b in zip(take, put):
            a.wait()
            b.start()
        g.come("a")

    def on(n):
        return lambda: z.go(n)

    happen(t, "-", {"0-": begin, "1-": serial(first, on("1")), "2-": serial(g.near, on("2"), come(g, "8")), "3-": serial(g.late, on("3"), come(g, "f")),
                    "4-": serial(g.last, on("4"), come(g, "6")), "5-": serial(on("5"), come(g, "e")), "6-": serial(on("6"), come(g, "c")),
                    "7-": serial(on("7"), come(g, "g"))})

    @pl.when(lax.rem(t, 4) == 0)
    def _():
        dk_s[...] = jnp.zeros_like(dk_s)
        dv_s[...] = jnp.zeros_like(dv_s)

    dh = dh_s[pl.ds(pl.multiple_of((seq * 4 + iq) * bq, bq), bq), :]
    dq_s[...] = jnp.zeros_like(dq_s)
    do_s[...] = nt(dh, wo_ref[...]).astype(BF16)
    go_s[...] += nn(o_ref[...].T, dh)
    parts = [slice(n * HEAD, (n + 1) * HEAD) for n in range(heads)]
    lses, deltas = [], []
    for n, c in enumerate(parts):
        lses.append(lse_ref[n : n + 1, :] * LOG2E)
        deltas.append((do_s[:, c].astype(F32) * o_ref[:, c].astype(F32)).T.sum(axis=0, keepdims=True))

    def tile(first, keys, q0, masked):
        here = pl.ds(pl.multiple_of(first, keys), keys)
        scores = [nt(k_ref[here, c], q_ref[q0:, c]) for c in parts]
        dps = [nt(v_ref[here, c], do_s[q0:, c]) for c in parts]
        if masked:
            shape = (keys, bq - q0)
            ok = lax.broadcasted_iota(jnp.int32, shape, 1) >= lax.broadcasted_iota(jnp.int32, shape, 0)
        for n, c in enumerate(parts):
            p = jnp.exp2(scores[n] * e - lses[n][:, q0:])
            if masked:
                p = jnp.where(ok, p, 0.0)
            ds = (p * (dps[n] - deltas[n][:, q0:])).astype(BF16)
            dv_s[n, here, :] += nn(p.astype(BF16), do_s[q0:, c])
            dk_s[n, here, :] += nn(ds, q_ref[q0:, c])
            dq_s[n, :, q0:] += nn(k_ref[here, c].T, ds)

    lax.fori_loop(0, iq, lambda j, _: tile(j * bq, bq, 0, False), None)
    for q0 in range(0, bq, bk):
        tile(iq * bq + q0, bk, q0, True)

    def back(a, cos, sin):
        a = a * scale
        return (a * cos - pltpu.roll(a, HEAD // 2, 1) * sin).astype(BF16)

    for n, c in enumerate(parts):
        dq_ref[:, c] = back(dq_s[n].T, cos_ref[...], sin_ref[...])

    @pl.when(lax.rem(t, 4) == 3)
    def _():
        for n, c in enumerate(parts):
            dk_ref[:, c] = back(dk_s[n], cosw_ref[...], sinw_ref[...])
            dv_ref[:, c] = dv_s[n].astype(BF16)

    @pl.when(t == pl.num_programs(0) - 1)
    def _():
        go_ref[...] = go_s[...].astype(BF16)
        for copy in put:
            copy.wait()
        z.come("01234567")
        g.sent()
        z.sent()


def attend_back(qkvs, o, own, lse, wo, cos, sin, gg, gu, n, bk=256):
    _, seqs, tokens, cols = qkvs.shape
    piece, d = own.shape
    bq, heads, half, wide = 2 * piece, cols // HEAD, gg.shape[0] // 2, gg.shape[1]
    at = lambda t: turn_of(BACK)(t)
    block = pl.BlockSpec((None, bq, cols), lambda t: (*at(t), 0))
    every = pl.BlockSpec((None, tokens, cols), lambda t: (at(t)[0], 0, 0))
    table = pl.BlockSpec((bq, HEAD), lambda t: (at(t)[1], 0))
    return pl.pallas_call(
        functools.partial(_attend_back, scale=HEAD**-0.5, bk=bk),
        grid=(len(BACK),),
        in_specs=[*three(at, tokens, bq, cols), block, whole(piece, d),
                  pl.BlockSpec((None, heads, bq), lambda t: (at(t)[0], 0, at(t)[1])), whole(cols, d), table, table, whole(tokens, HEAD), whole(tokens, HEAD), ANY, ANY],
        out_specs=[block, every, every, whole(cols, d), ANY, ANY],
        out_shape=[jax.ShapeDtypeStruct((seqs, tokens, cols), BF16)] * 3 + [jax.ShapeDtypeStruct((cols, d), BF16)] +
                  [jax.ShapeDtypeStruct((half, 2 * wide), BF16)] * 2,
        scratch_shapes=[pltpu.VMEM((seqs * tokens, d), BF16), pltpu.VMEM((bq, cols), BF16), pltpu.VMEM((heads, HEAD, bq), F32), pltpu.VMEM((heads, tokens, HEAD), F32),
                        pltpu.VMEM((heads, tokens, HEAD), F32), pltpu.VMEM((cols, d), F32), pltpu.VMEM((2, half, wide), BF16)] + sems(N_MSG + 8) +
                       [pltpu.SemaphoreType.DMA((2,))],
        compiler_params=comm_params(n), name="attend_back",
        cost_estimate=pl.CostEstimate(flops=10 * seqs * tokens * tokens * cols, transcendentals=0, bytes_accessed=16 * seqs * tokens * cols),
    )(qkvs, qkvs, qkvs, o, own, lse, wo, cos, sin, cos, sin, gg, gu)


LAST = kinds("1614121006040200")


def _qkv_back(x_ref, dh_ref, w_ref, at_ref, dq_ref, dk_ref, dv_ref, dx_ref, gq_ref, gk_ref, gv_ref,
              at_s, g_s, sum_s, low_s, da_s, peer, out, diag, block, across, send, recv, local, given, more):
    place = Place(x_ref.shape[0])
    both, half, cols, tokens = 2 * place.piece, gq_ref.shape[0], sum_s.shape[1], at_s.shape[1]
    s = Sum(place, da_s, peer, out, diag, block, across, send, recv)
    theirs, mine = (pl.ds(pl.multiple_of(p * half, half), half) for p in (1 - place.p, place.p))
    at = pl.ds(pl.multiple_of(place.p * cols, cols), cols)
    outs = (gq_ref, gk_ref, gv_ref)
    z = Swap(place, send, recv, N_MSG, [(low_s.at[n, theirs], o.at[:, at]) for n, o in enumerate(outs)])
    keep = [pltpu.make_async_copy(low_s.at[n, mine], o.at[:, at], local.at[n]) for n, o in enumerate(outs)]
    deep = tokens // 4
    parts = [pl.ds(c * deep, deep) for c in range(4)]
    loads = [pltpu.make_async_copy(at_ref.at[:, c], at_s.at[:, c], given.at[2 * n]) for n, c in enumerate(parts)]
    loadq = [pltpu.make_async_copy(dq_ref.at[c], g_s.at[0, c], given.at[2 * n + 1]) for n, c in enumerate(parts)]
    loadkv = [pltpu.make_async_copy(o, g_s.at[n + 1], more.at[n]) for n, o in enumerate((dk_ref, dv_ref))]
    for pair in zip(loads, loadq):
        for copy in pair:
            copy.start()
    for copy in loadkv:
        copy.start()
    place.greet()

    def give(m):
        low_s[m] = sum_s[...].astype(BF16)
        z.go(str(m))
        keep[m].start()

    def whole_of(m):
        sum_s[...] = jnp.zeros_like(sum_s)

        def go(n, _):
            here = pl.ds(pl.multiple_of(n * deep, deep), deep)
            sum_s[...] += nn(at_s[:, here], g_s[m, here, :])

        lax.fori_loop(0, 4, go, None)
        give(m)

    for n, c in enumerate(parts):
        loads[n].wait()
        loadq[n].wait()
        term = nn(at_s[:, c], g_s[0, c, :])
        sum_s[...] = sum_s[...] + term if n else term
    give(0)
    for copy in loadkv:
        copy.wait()

    def step(n, _):
        seq, chip = turn_of(LAST)(n)
        rows = pl.ds(pl.multiple_of((seq * 4 + chip) * both, both), both)
        da_s[rows, :] = (nt(g_s[0, rows, :], w_ref[0]) + nt(g_s[1, rows, :], w_ref[1]) + nt(g_s[2, rows, :], w_ref[2])).astype(BF16)
        for k, kind in enumerate(LAST):
            pl.when(n == k)(functools.partial(s.start, *kind))
        happen(n, "-", {"2": calls(s.deal, LAST[0]), "6": calls(s.deal, LAST[4])})

    half_way = len(LAST) // 2
    lax.fori_loop(0, half_way, step, None)
    whole_of(1)
    for kind in kinds("1412"):
        s.deal(*kind)
    lax.fori_loop(half_way, len(LAST), step, None)
    whole_of(2)
    for kind in kinds("10040200"):
        total = s.deal(*kind)
    dx_ref[...] = (dh_ref[...].astype(F32) + norm_back(x_ref[...], total)).astype(BF16)
    for copy in keep:
        copy.wait()
    z.come("012")
    z.sent()
    s.sent()


def qkv_back(at, dq, dk, dv, w, x, dh, n):
    piece, d = x.shape
    tokens, cols = dq.shape
    return pl.pallas_call(
        _qkv_back,
        in_specs=[IN_VMEM] * 3 + [ANY] * 4,
        out_specs=[IN_VMEM] + [ANY] * 3,
        out_shape=[jax.ShapeDtypeStruct((piece, d), BF16)] + [jax.ShapeDtypeStruct((d // 2, 2 * cols), BF16)] * 3,
        scratch_shapes=[pltpu.VMEM((d, tokens), BF16), pltpu.VMEM((3, tokens, cols), BF16), pltpu.VMEM((d, cols), F32), pltpu.VMEM((3, d, cols), BF16),
                        pltpu.VMEM((tokens, d), BF16)] + sum_scratch(piece, d) + sems(N_MSG + 3) + [pltpu.SemaphoreType.DMA((n,)) for n in (3, 8, 2)],
        compiler_params=comm_params(n), name="qkv_back",
        cost_estimate=pl.CostEstimate(flops=12 * tokens * d * cols, transcendentals=0, bytes_accessed=8 * tokens * cols),
    )(x, dh, w, at, dq, dk, dv)


def _settle(*refs):
    n = len(refs) // 3
    ins, outs, held, sem = refs[:n], refs[n : 2 * n], refs[2 * n : 3 * n], refs[-1]
    take = [pltpu.make_async_copy(a, b, sem.at[k]) for k, (a, b) in enumerate(zip(ins, held))]
    put = [pltpu.make_async_copy(b, c, sem.at[k]) for k, (b, c) in enumerate(zip(held, outs))]
    for copy in take:
        copy.start()
    for a, b in zip(take, put):
        a.wait()
        b.start()
    for copy in put:
        copy.wait()


def settle(arrays):
    n = len(arrays)
    return pl.pallas_call(
        _settle,
        in_specs=[ANY] * n, out_specs=[ANY] * n, out_shape=[jax.ShapeDtypeStruct(a.shape, a.dtype) for a in arrays],
        scratch_shapes=[pltpu.VMEM(a.shape, a.dtype) for a in arrays] + [pltpu.SemaphoreType.DMA((n,))],
        compiler_params=pltpu.CompilerParams(vmem_limit_bytes=VMEM), name="settle")(*arrays)


def solution(mesh):
    def step(x, dy, wq, wk, wv, wo, wg, wu, wd):
        x, dy = x[0], dy[0]
        qkvs, at, w, got0, dys, hide, cos, sin = qkv(x, dy, wd, wq, wk, wv, wg, 8 * x.shape[0], 0)
        qkvs = qkvs.reshape(3, 2, -1, qkvs.shape[-1])
        o, lse, h, b, got1, got2 = attend(qkvs, wo, x, wg, wu, 1)
        dh, gg, gu, gd = units(b, h, dy, dys, hide, (wg, wu, got0, got1, got2), 2)
        dq, dk, dv, go, gg, gu = attend_back(qkvs, o, dh, lse, wo, cos, sin, gg, gu, 3)
        dq, dk, dv = (t.reshape(-1, t.shape[-1]) for t in (dq, dk, dv))
        dx, gq, gk, gv = qkv_back(at, dq, dk, dv, w, x, dh, 4)
        gd, gg, gu, go, gq, gk, gv, dx = settle([gd, gg, gu, go, gq, gk, gv, dx])
        return dx[None], gq, gk, gv, go, gg, gu, gd

    states, by_columns, by_rows = P("dp", "tp", None), P("dp", "tp"), P(("tp", "dp"), None)
    weights = (by_columns, by_columns, by_columns, by_rows, by_columns, by_columns, by_rows)
    return jax.shard_map(step, mesh=mesh, in_specs=(states, states, *weights), out_specs=(states, *weights), check_vma=False)
```

```python
import functools

import jax
import jax.numpy as jnp
import numpy as np
from jax import lax
from jax.experimental import pallas as pl
from jax.experimental.pallas import tpu as pltpu
from jax.sharding import PartitionSpec as P

NEG = -1e30
HIDDEN = 2 * NEG
LOG2E = 1.4426950408889634
VMEM = 60 * 2**20
HEAD = 128
THETA = 10000
EPS = 1e-6
F32, BF16 = jnp.float32, jnp.bfloat16


def _dot(a, b, ca, cb):
    return lax.dot_general(a, b, (((ca,), (cb,)), ((), ())), preferred_element_type=F32)


def nn(a, b):
    return _dot(a, b, 1, 0)


def nt(a, b):
    return _dot(a, b, 1, 1)


FINE = 32


def tables(tokens):
    half = HEAD // 2
    out = []
    for places in (np.arange(0, tokens, FINE), np.arange(FINE)):
        angle = places[:, None] * float(THETA) ** (-np.arange(half) / half)
        cos, sin = np.cos(angle), np.sin(angle)
        out += [np.concatenate(pair, -1).astype(np.float32) for pair in ((cos, cos), (-sin, sin))]
    return [jnp.asarray(t) for t in out]


def normed(h):
    wide = h.astype(F32)
    scale = lax.rsqrt(jnp.mean(wide**2, -1, keepdims=True) + EPS)
    return (wide * scale).astype(BF16)


def norm_back(h, d):
    wide = h.astype(F32)
    scale = lax.rsqrt(jnp.mean(wide**2, -1, keepdims=True) + EPS)
    return scale * d - wide * (scale**3 * jnp.mean(d * wide, -1, keepdims=True))


MESH = pl.DeviceIdType.MESH
N_MSG = 17


def read(code):
    dz, flip, half = code
    return int(dz), int(flip), None if half == "-" else int(half)


def by(text, like):
    return [text[n : n + len(like)] for n in range(0, len(text), len(like))]


def kinds(text):
    return [(int(dz), int(flip)) for dz, flip in by(text, "--")]


def numbers(text):
    return [int(c, N_MSG) for c in text]


class Place:
    def __init__(self, piece):
        self.p, self.i = lax.axis_index("dp"), lax.axis_index("tp")
        self.piece = piece
        self.x, self.y, self.z, self.c = (self.p, self.i ^ 4), (self.p, self.i ^ 2), (1 - self.p, self.i), (self.p, self.i ^ 1)

    def rows(self, dz, flip, half=None):
        n = self.piece
        at = ((1 - self.p if dz else self.p) * 8 + (self.i ^ flip)) * n
        if half is None:
            return pl.ds(pl.multiple_of(at, n), n)
        return pl.ds(pl.multiple_of(at + half * (n // 2), n // 2), n // 2)

    def greet(self):
        barrier = pltpu.get_barrier_semaphore()
        for who in (self.x, self.y, self.z, self.c):
            pl.semaphore_signal(barrier, inc=1, device_id=who, device_id_type=MESH)
        pl.semaphore_wait(barrier, 4)


class Gather:
    COMES = [read(c) for c in by("10-04-02-01-14-12-11-06005-06103-16015-16113-07-17-", "---")]
    GOES = [(c[:1], *read(c[1:])) for c in by("z00-x00-y00-c00-x10-y10-c10-y040c04-x021c02-", "----") + by("y140c14-x121c12-c06-c16-", "----")]

    def __init__(self, place, all_ref, send, recv, first=0):
        self.place, self.all_ref, self.send, self.recv, self.first = place, all_ref, send, recv, first

    def copy(self, m, rows):
        src = self.all_ref.at[rows]
        return pltpu.make_async_remote_copy(src_ref=src, dst_ref=src, send_sem=self.send.at[self.first + m], recv_sem=self.recv.at[self.first + m],
                                            device_id=getattr(self.place, self.GOES[m][0]), device_id_type=MESH)

    def go(self, ms):
        for m in numbers(ms):
            self.copy(m, self.place.rows(*self.GOES[m][1:])).start()

    def come(self, ms):
        for m in numbers(ms):
            self.copy(m, self.place.rows(*self.COMES[m])).wait_recv()

    def start(self):
        self.go("1203")

    def beside(self):
        self.come("1")
        self.go("78")
        self.come("2")
        self.go("9a")

    def beyond(self):
        self.come("0")
        self.go("456")

    def middle(self):
        self.beside()
        self.beyond()

    def near(self):
        self.come("79")
        self.go("f")

    def late(self):
        self.come("4")
        self.go("bc")
        self.come("5")
        self.go("de")

    def last(self):
        self.come("bd")
        self.go("g")

    def sent(self):
        for m in range(N_MSG):
            self.copy(m, self.place.rows(*self.GOES[m][1:])).wait_send()


class Sum:
    KINDS = kinds("1614121006040200")

    def __init__(self, place, part_ref, peer, out, diag, block, across, send, recv, first=0):
        self.place, self.part_ref, self.peer, self.out, self.diag, self.block, self.across = place, part_ref, peer, out, diag, block, across
        self.send, self.recv, self.first = send, recv, first

    def copy(self, m, src, dst, who):
        return pltpu.make_async_remote_copy(src_ref=src, dst_ref=dst, send_sem=self.send.at[self.first + m], recv_sem=self.recv.at[self.first + m],
                                            device_id=who, device_id_type=MESH)

    def to_peer(self, k):
        dz, f = self.KINDS[k]
        return self.copy(k, self.part_ref.at[self.place.rows(dz, f ^ 1)], self.peer.at[k], self.place.c)

    def to_diag(self, dz, way):
        k, h = self.KINDS.index((dz, 6)), self.place.piece // 2
        return self.copy(8 + 2 * dz + way, self.out.at[k, pl.ds(way * h, h)], self.diag.at[dz, way], self.place.y if way else self.place.x)

    def to_block(self, dz, way):
        k = self.KINDS.index((dz, 2 if way else 4))
        return self.copy(12 + 2 * dz + way, self.out.at[k], self.block.at[dz, way], self.place.y if way else self.place.x)

    def to_z(self):
        return self.copy(16, self.out.at[self.KINDS.index((1, 0))], self.across, self.place.z)

    def both(self, k, half=None):
        dz, f = self.KINDS[k]
        self_rows = self.place.rows(dz, f, half)
        h = self.place.piece // 2
        mine = self.part_ref[self_rows, :].astype(F32)
        return mine + (self.peer[k] if half is None else self.peer[k, half * h : (half + 1) * h]).astype(F32)

    def start(self, dz, f):
        self.to_peer(self.KINDS.index((dz, f))).start()

    def deal(self, dz, f):
        k = self.KINDS.index((dz, f))
        h = self.place.piece // 2
        self.to_peer(k).wait_recv()
        if f == 6:
            self.out[k] = self.both(k).astype(BF16)
            self.to_diag(dz, 0).start()
            self.to_diag(dz, 1).start()
        elif f:
            way = 1 if f == 2 else 0
            self.to_diag(dz, 1 - way).wait_recv()
            joint = 1 - way
            self.out[k, joint * h : (joint + 1) * h] = (self.both(k, joint) + self.diag[dz, joint].astype(F32)).astype(BF16)
            self.out[k, way * h : (way + 1) * h] = self.both(k, way).astype(BF16)
            self.to_block(dz, way).start()
        else:
            self.to_block(dz, 0).wait_recv()
            self.to_block(dz, 1).wait_recv()
            total = self.both(k) + self.block[dz, 0].astype(F32) + self.block[dz, 1].astype(F32)
            if not dz:
                self.to_z().wait_recv()
                return total + self.across[...].astype(F32)
            self.out[k] = total.astype(BF16)
            self.to_z().start()

    def sent(self):
        for k in range(8):
            self.to_peer(k).wait_send()
        for dz in range(2):
            for way in range(2):
                self.to_diag(dz, way).wait_send()
                self.to_block(dz, way).wait_send()
        self.to_z().wait_send()


def sum_scratch(piece, d):
    return [pltpu.VMEM((8, piece, d), BF16), pltpu.VMEM((8, piece, d), BF16), pltpu.VMEM((2, 2, piece // 2, d), BF16),
            pltpu.VMEM((2, 2, piece, d), BF16), pltpu.VMEM((piece, d), BF16)]


def sems(n):
    return [pltpu.SemaphoreType.DMA((n,)), pltpu.SemaphoreType.DMA((n,))]


def comm_params(n):
    return pltpu.CompilerParams(collective_id=n, has_side_effects=True, vmem_limit_bytes=VMEM)


def three(at, tokens, bq, cols):
    every = lambda which: pl.BlockSpec((None, None, tokens, cols), lambda t: (which, at(t)[0], 0, 0))
    return pl.BlockSpec((None, None, bq, cols), lambda t: (0, *at(t), 0)), every(1), every(2)


class Swap:
    def __init__(self, place, send, recv, first, what):
        self.place, self.send, self.recv, self.first, self.what = place, send, recv, first, what

    def copy(self, n):
        src, dst = self.what[n]
        return pltpu.make_async_remote_copy(src_ref=src, dst_ref=dst, send_sem=self.send.at[self.first + n], recv_sem=self.recv.at[self.first + n],
                                            device_id=self.place.z, device_id_type=MESH)

    def go(self, ns):
        for n in numbers(ns):
            self.copy(n).start()

    def come(self, ns):
        for n in numbers(ns):
            self.copy(n).wait_recv()

    def sent(self):
        for n in range(len(self.what)):
            self.copy(n).wait_send()


def bit(t, bits):
    return (np.int32(np.array(sum(b << n for n, b in enumerate(bits)), np.uint32).view(np.int32)) >> t) & 1


def pick(t, values):
    return bit(t, [v & 1 for v in values]) + 2 * bit(t, [v >> 1 for v in values])


def turn_of(kinds):
    p, i = lax.axis_index("dp"), lax.axis_index("tp")
    return lambda t: (p ^ bit(t, [dz for dz, _ in kinds]), (i // 2) ^ pick(t, [f // 2 for _, f in kinds]))


def whole(*shape):
    return pl.BlockSpec(shape, lambda *t: (0,) * len(shape), pipeline_mode=pl.Buffered(1))


def happen(t, at, events):
    for when, fn in events.items():
        if when[1:] in ("", at):
            pl.when(t == int(when[0]))(fn)


def serial(*fns):
    def go():
        for fn in fns:
            fn()

    return go


def come(g, ms):
    return lambda: g.come(ms)


def calls(fn, *args):
    def go():
        for arg in args:
            fn(*arg)

    return go


ANY, IN_VMEM = pl.BlockSpec(memory_space=pl.ANY), pl.BlockSpec(memory_space=pltpu.VMEM)
CHUNK = 512
EARLY = 2 * CHUNK


def chunks(src, dst, to, at, cols):
    return [(src.at[:, pl.ds(pl.multiple_of(to + c, CHUNK), CHUNK)], dst.at[:, pl.ds(pl.multiple_of(at + c, CHUNK), CHUNK)]) for c in range(0, cols, CHUNK)]


FIRST = kinds("0010020406141216")
HIDE = kinds("0002041006141216")


def _qkv(own_ref, dyo_ref, cos0_ref, sin0_ref, cos1_ref, sin1_ref, wdin_ref, wq_ref, wk_ref, wv_ref, wg_ref,
         out_ref, at_ref, wout_ref, got_ref, dy_ref, hide_ref, cosout_ref, sinout_ref,
         x_s, a_s, at_s, out_s, w_s, dy_s, hide_s, wd_ref, cos_ref, sin_ref, send, recv, local, loaded):
    place = Place(own_ref.shape[0])
    tokens, cols = cos_ref.shape[0], w_s.shape[2]
    both, half, wide = 2 * place.piece, wq_ref.shape[0], wg_ref.shape[1] // 2
    g = Gather(place, x_s, send, recv)
    mine = pl.ds(pl.multiple_of(place.p * half, half), half)
    weights = (wq_ref, wk_ref, wv_ref)
    there = [(w.at[:, pl.ds(pl.multiple_of((1 - place.p) * cols, cols), cols)], w_s.at[k, mine]) for k, w in enumerate(weights)]
    there += chunks(wg_ref, got_ref, (1 - place.p) * wide, 0, EARLY)
    z = Swap(place, send, recv, 2 * N_MSG, there)
    d = Gather(place, dy_s, send, recv, N_MSG)
    here = [pltpu.make_async_copy(w.at[:, pl.ds(pl.multiple_of(place.p * cols, cols), cols)], w_s.at[k, mine], local.at[k]) for k, w in enumerate(weights)]
    load = [pltpu.make_async_copy(*pair, loaded.at[k]) for k, pair in enumerate([(wdin_ref, wd_ref)])]
    for copy in load + here:
        copy.start()
    place.greet()
    x_s[place.rows(0, 0), :] = own_ref[...]
    dy_s[place.rows(0, 0), :] = dyo_ref[...]
    g.start()
    z.go("01")
    d.go("03")
    z.go("234")

    def turns(n, _):
        rows = pl.ds(pl.multiple_of(n * FINE, FINE), FINE)
        cos, sin = cos0_ref[pl.ds(n, 1), :], sin0_ref[pl.ds(n, 1), :]
        cos_ref[rows, :] = cos * cos1_ref[...] - sin * sin1_ref[...]
        sin_ref[rows, :] = sin * cos1_ref[...] + cos * sin1_ref[...]

    lax.fori_loop(0, tokens // FINE, turns, None)
    table_copies = [pltpu.make_async_copy(*pair, loaded.at[k + 1]) for k, pair in enumerate([(cos_ref, cosout_ref), (sin_ref, sinout_ref)])]
    for copy in table_copies:
        copy.start()

    def hide(rows):
        for c in range(0, hide_s.shape[1], CHUNK):
            hide_s[rows, c : c + CHUNK] = nt(dy_s[rows, :], wd_ref[c : c + CHUNK, :]).astype(BF16)
        pltpu.make_async_copy(hide_s.at[rows], hide_ref.at[rows], local.at[5]).start()
        pltpu.make_async_copy(dy_s.at[rows], dy_ref.at[rows], local.at[6]).start()

    def result(m, rows, a):
        t = nn(a, w_s[m]).astype(BF16)
        if m < 2:
            here = pl.ds(pl.multiple_of(lax.rem(rows.start, tokens), both), both)
            cos, sin = cos_ref[here, :], sin_ref[here, :]
            for at in range(0, cols, HEAD):
                one = t[:, at : at + HEAD].astype(F32)
                out_s[m, rows, at : at + HEAD] = (one * cos + pltpu.roll(one, HEAD // 2, 1) * sin).astype(BF16)
        else:
            out_s[m, rows, :] = t
        pltpu.make_async_copy(out_s.at[m, rows], out_ref.at[m, rows], local.at[m]).start()

    def first(rows):
        a = normed(x_s[rows, :])
        a_s[rows, :] = a
        at_s[:, rows] = a.T
        result(0, rows, a)

    def later(m):
        return lambda rows: result(m, rows, a_s[rows, :])

    at_copy = pltpu.make_async_copy(at_s, at_ref, local.at[3])
    w_copy = pltpu.make_async_copy(w_s, wout_ref, local.at[4])

    def loads():
        for copy in here:
            copy.wait()

    ways = {"h": (hide, HIDE, zip("1234567", "a86fceg"), d), "q": (first, FIRST, zip("1234567", "6a8fceg"), g), "k": (later(1), FIRST, (), None),
            "v": (later(2), FIRST, (), None)}
    ways = {name: (fn, order, list(needs), who) for name, (fn, order, needs, who) in ways.items()}

    def run(code):
        name, a, b = code
        fn, order, needs, who = ways[name]

        def one(n, _):
            for at, ms in needs:
                if a <= at < b:
                    pl.when(n == int(at))(come(who, ms))
            seq, chip = turn_of(order)(n)
            fn(pl.ds(pl.multiple_of((seq * 4 + chip) * both, both), both))

        lax.fori_loop(int(a), int(b), one, None)

    d.come("3")
    load[0].wait()
    run("h01")
    g.middle()
    d.go("12")
    g.near()
    loads()
    z.come("0")
    g.come("3")
    run("q05")
    g.late()
    run("q57")
    z.come("1")
    run("k07")
    d.beside()
    run("h13")
    g.last()
    run("q78")
    at_copy.start()
    run("k78")
    d.beyond()
    d.near()
    run("h35")
    z.come("2")
    w_copy.start()
    run("v08")
    d.late()
    d.last()
    run("h58")
    at_copy.wait()
    w_copy.wait()
    for m in range(3):
        pltpu.make_async_copy(out_s.at[m], out_ref.at[m], local.at[m]).wait()
    z.come("34")
    g.sent()
    d.sent()
    z.sent()
    for copy in table_copies:
        copy.wait()
    pltpu.make_async_copy(hide_s, hide_ref, local.at[5]).wait()
    pltpu.make_async_copy(dy_s, dy_ref, local.at[6]).wait()


def qkv(own, dy, wd, wq, wk, wv, wg, tokens, n):
    piece, d = own.shape
    given, table = tables(tokens), (tokens, HEAD)
    tokens, cols, half = 16 * piece, wq.shape[1] // 2, wq.shape[0]
    shapes = [(3, tokens, cols), (d, tokens), (3, d, cols), (half, EARLY), (tokens, d), (tokens, wd.shape[0])]
    return pl.pallas_call(
        _qkv,
        in_specs=[IN_VMEM] * 6 + [ANY] * 5,
        out_specs=[ANY] * 8,
        out_shape=[jax.ShapeDtypeStruct(shape, BF16) for shape in shapes] + [jax.ShapeDtypeStruct(table, F32)] * 2,
        scratch_shapes=[pltpu.VMEM(shape, BF16) for shape in [(tokens, d)] * 2 + [(d, tokens), (3, tokens, cols), (3, d, cols), *shapes[4:], wd.shape]] +
                       [pltpu.VMEM(table, F32)] * 2 + sems(2 * N_MSG + 5) + [pltpu.SemaphoreType.DMA((7,)), pltpu.SemaphoreType.DMA((3,))],
        compiler_params=comm_params(n), name="qkv",
        cost_estimate=pl.CostEstimate(flops=6 * tokens * d * cols, transcendentals=0, bytes_accessed=8 * tokens * cols),
    )(own, dy, *given, wd, wq, wk, wv, wg)


def _attend(q_ref, k_ref, v_ref, wo_ref, x_ref, wg_ref, wu_ref, o_ref, lse_ref, h_ref, b_ref, gotg_ref, gotu_ref,
            top_s, mix_s, term_s, peer, out, diag, block_s, across, send, recv, *, scale, bk):
    t = pl.program_id(0)
    place = Place(x_ref.shape[0])
    bq, width = q_ref.shape
    heads, wide = width // HEAD, wg_ref.shape[1] // 2
    seq, iq = turn_of(Sum.KINDS)(t)
    e = scale * LOG2E
    s = Sum(place, term_s, peer, out, diag, block_s, across, send, recv)
    other = (1 - place.p) * wide
    there = chunks(wg_ref, gotg_ref, other + EARLY, 0, wide - EARLY) + chunks(wu_ref, gotu_ref, other, 0, wide - CHUNK)
    z = Swap(place, send, recv, N_MSG, there)

    def begin():
        place.greet()
        z.go("01")

    def deal(n):
        return calls(s.deal, Sum.KINDS[n])

    def on(n):
        return lambda: z.go(n)

    events = {"0-": begin, "1-": on("2"), "2-": on("3"), "5-": on("4")}
    events |= {when: deal(n) for n, when in enumerate(by("1+2+3+6-5+6+7+", "--"))}
    happen(t, "-", events)

    pieces = [slice(n * HEAD, (n + 1) * HEAD) for n in range(heads)]
    top_s[...] = jnp.full(top_s.shape, NEG, F32)
    mix_s[...] = jnp.zeros(mix_s.shape, F32)
    def tile(first, keys, q0, masked):
        here = pl.ds(pl.multiple_of(first, keys), keys)
        scores = [nt(k_ref[here, c], q_ref[q0:, c]) for c in pieces]
        if masked:
            shape = (keys, bq - q0)
            ok = lax.broadcasted_iota(jnp.int32, shape, 1) >= lax.broadcasted_iota(jnp.int32, shape, 0)
        weights, keeps = [], []
        for i, score in enumerate(scores):
            if masked:
                score = jnp.where(ok, score, HIDDEN)
            old = top_s[i : i + 1, q0:]
            top = jnp.maximum(old, score.max(axis=0, keepdims=True))
            top_s[i : i + 1, q0:] = top
            weights.append(jnp.exp2((score - top) * e).astype(BF16))
            keeps.append(jnp.exp2((old - top) * e))
        ones = jnp.ones((8, keys), BF16)
        for i, (c, p, keep) in enumerate(zip(pieces, weights, keeps)):
            values = jnp.concatenate([v_ref[here, c].T, ones], axis=0)
            mix_s[i, :, q0:] = mix_s[i, :, q0:] * keep + nn(values, p)

    lax.fori_loop(0, iq, lambda j, _: tile(j * bq, bq, 0, False), None)
    happen(t, "+", events)
    for q0 in range(0, bq, bk):
        tile(iq * bq + q0, bk, q0, True)
    for i, c in enumerate(pieces):
        top, total = top_s[i : i + 1, :], mix_s[i, HEAD : HEAD + 1, :]
        o_ref[:, c] = (mix_s[i, :HEAD, :] * (1 / total)).T.astype(BF16)
        lse_ref[i : i + 1, :] = top * scale + jnp.log(total)
    term_s[pl.ds(pl.multiple_of((seq * 4 + iq) * bq, bq), bq), :] = nn(o_ref[...], wo_ref[...]).astype(BF16)
    for step, kind in enumerate(Sum.KINDS):
        pl.when(t == step)(functools.partial(s.start, *kind))

    @pl.when(t == pl.num_programs(0) - 1)
    def _():
        total = s.deal(*Sum.KINDS[-1])
        h = (x_ref[...].astype(F32) + total).astype(BF16)
        h_ref[...] = h
        b_ref[...] = normed(h)
        z.come("01234")
        s.sent()
        z.sent()


def attend(qkvs, wo, x, wg, wu, n, bk=256):
    _, seqs, tokens, cols = qkvs.shape
    piece, d = x.shape
    bq, heads, half, wide = 2 * piece, cols // HEAD, wg.shape[0], wg.shape[1] // 2
    at = lambda t: turn_of(Sum.KINDS)(t)
    return pl.pallas_call(
        functools.partial(_attend, scale=HEAD**-0.5, bk=bk),
        grid=(len(Sum.KINDS),),
        in_specs=[*three(at, tokens, bq, cols), whole(cols, d), whole(piece, d), ANY, ANY],
        out_specs=[pl.BlockSpec((None, bq, cols), lambda t: (*at(t), 0)), pl.BlockSpec((None, heads, bq), lambda t: (at(t)[0], 0, at(t)[1])),
                   whole(piece, d), whole(piece, d), ANY, ANY],
        out_shape=[jax.ShapeDtypeStruct((seqs, tokens, cols), BF16), jax.ShapeDtypeStruct((seqs, heads, tokens), F32)] +
                  [jax.ShapeDtypeStruct((piece, d), BF16)] * 2 + [jax.ShapeDtypeStruct((half, wide - EARLY), BF16), jax.ShapeDtypeStruct((half, wide - CHUNK), BF16)],
        scratch_shapes=[pltpu.VMEM((8, bq), F32), pltpu.VMEM((heads, HEAD + 8, bq), F32), pltpu.VMEM((seqs * tokens, d), BF16)] + sum_scratch(piece, d) +
                       sems(N_MSG + 5),
        compiler_params=comm_params(n), name="attend",
        cost_estimate=pl.CostEstimate(flops=4 * seqs * tokens * tokens * cols, transcendentals=0, bytes_accessed=10 * seqs * tokens * cols),
    )(qkvs, qkvs, qkvs, wo, x, wg, wu)


STEPS = kinds("0004101614120602")


def _units(own_ref, h_ref, dyo_ref, dy_ref, hide_ref, gate_ref, up_ref, got0_ref, got1_ref, got2_ref, dh_ref, gg_ref, gu_ref, gd_ref,
           wg_ref, wu_ref, b_s, db_s, g_s, u_s, d_s, low_s, last_s, peer, out, diag, block, across, send, recv, local, *, wide):
    t = pl.program_id(0)
    place = Place(own_ref.shape[0])
    both = 2 * place.piece
    g = Gather(place, b_s, send, recv)
    s = Sum(place, db_s, peer, out, diag, block, across, send, recv, N_MSG)

    half, ff = gate_ref.shape[0], wg_ref.shape[1]
    mine, theirs = (pl.ds(pl.multiple_of(p * half, half), half) for p in (place.p, 1 - place.p))
    cols = pl.ds(pl.multiple_of(place.p * ff, ff), ff)
    loads = [(gate_ref.at[:, cols], wg_ref.at[mine]), (up_ref.at[:, cols], wu_ref.at[mine]), (got2_ref, wu_ref.at[theirs, pl.ds(0, ff - CHUNK)]),
             (got0_ref, wg_ref.at[theirs, pl.ds(0, EARLY)]), (got1_ref, wg_ref.at[theirs, pl.ds(EARLY, ff - EARLY)])]
    other = pl.ds(pl.multiple_of((2 - place.p) * ff - CHUNK, CHUNK), CHUNK)
    z = Swap(place, send, recv, 2 * N_MSG, [(up_ref.at[:, other], wu_ref.at[mine, pl.ds(ff - CHUNK, CHUNK)])])
    loads = [pltpu.make_async_copy(*pair, local.at[n]) for n, pair in enumerate(loads)]

    def begin():
        for copy in loads:
            copy.start()
        place.greet()
        b_s[place.rows(0, 0), :] = own_ref[...]
        z.go("0")
        g.start()
        for acc in (g_s, u_s, d_s):
            acc[...] = jnp.zeros_like(acc)
        for copy in loads:
            copy.wait()
        g.come("3")

    def deal(text):
        return calls(s.deal, *kinds(text))

    def beside():
        g.beside()
        z.come("0")

    def beyond():
        g.near()
        g.beyond()

    events = {"00": begin, "03": beside, "10": come(g, "8"), "12": beyond, "20": come(g, "6"), "21": g.late, "23": g.last, "30": come(g, "g"),
              "40": come(g, "c"), "50": come(g, "e"), "60": come(g, "f"), "70": come(g, "a")}
    events |= {"42": deal("16"), "52": deal("14"), "62": deal("12"), "72": deal("0610")}
    seq, chip = turn_of(STEPS)(t)
    rows = pl.ds(pl.multiple_of((seq * 4 + chip) * both, both), both)
    db = bt = None
    for n, first in enumerate(range(0, wg_ref.shape[1], wide)):
        happen(t, str(n), events)
        if n == 0:
            b, dy = b_s[rows, :], dy_ref[...]
            bt, dyt = b.T, dy.T
        here = slice(first, first + wide)
        gate, up = nn(b, wg_ref[:, here]), nn(b, wu_ref[:, here])
        dhid = hide_ref[:, here].astype(F32)
        sig = 1 / (1 + jnp.exp2(gate * -LOG2E))
        silu = gate * sig
        hid = (silu * up).astype(BF16)
        du = (dhid * silu).astype(BF16)
        dg = (dhid * up * (sig + silu * (1 - sig))).astype(BF16)
        term = nt(dg, wg_ref[:, here]) + nt(du, wu_ref[:, here])
        db = term if db is None else db + term
        g_s[:, here] += nn(bt, dg)
        u_s[:, here] += nn(bt, du)
        d_s[:, here] += nn(dyt, hid)
    db_s[rows, :] = db.astype(BF16)
    for step, kind in enumerate(STEPS):
        pl.when(t == step)(functools.partial(s.start, *kind))

    @pl.when(t == len(STEPS) - 1)
    def _():
        s.deal(0, 2)
        s.deal(0, 4)
        low_s[0] = g_s[...].astype(BF16)
        low_s[1] = u_s[...].astype(BF16)
        last_s[...] = d_s[...].T.astype(BF16)
        saves = [pltpu.make_async_copy(*pair, local.at[k]) for k, pair in enumerate([(low_s.at[0], gg_ref), (low_s.at[1], gu_ref), (last_s, gd_ref)])]
        for copy in saves:
            copy.start()
        total = s.deal(0, 0)
        dh_ref[...] = (dyo_ref[...].astype(F32) + norm_back(h_ref[...], total)).astype(BF16)
        g.sent()
        s.sent()
        z.sent()
        for copy in saves:
            copy.wait()


def units(own, h, dyo, dy, hide, ws, n, wide=512):
    piece, d = own.shape
    tokens, ff = hide.shape
    at = lambda t: turn_of(STEPS)(t)
    return pl.pallas_call(
        functools.partial(_units, wide=wide),
        grid=(len(STEPS),),
        in_specs=[whole(piece, d)] * 3 + [pl.BlockSpec((2 * piece, width), lambda t: (at(t)[0] * 4 + at(t)[1], 0)) for width in (d, ff)] + [ANY] * 5,
        out_specs=[whole(piece, d)] + [ANY] * 3,
        out_shape=[jax.ShapeDtypeStruct((piece, d), BF16), jax.ShapeDtypeStruct((d, ff), BF16), jax.ShapeDtypeStruct((d, ff), BF16),
                   jax.ShapeDtypeStruct((ff, d), BF16)],
        scratch_shapes=[pltpu.VMEM((d, ff), BF16)] * 2 + [pltpu.VMEM((tokens, d), BF16)] * 2 + [pltpu.VMEM((d, ff), F32)] * 3 + [pltpu.VMEM((2, d, ff), BF16), pltpu.VMEM((ff, d), BF16)] + sum_scratch(piece, d) + sems(2 * N_MSG + 1) + [pltpu.SemaphoreType.DMA((5,))],
        compiler_params=comm_params(n),
        cost_estimate=pl.CostEstimate(flops=16 * tokens * d * ff, transcendentals=tokens * ff, bytes_accessed=6 * tokens * d + 12 * d * ff),
        name="units",
    )(own, h, dyo, dy, hide, *ws)


BACK = kinds("0002040610121416")


def _attend_back(q_ref, k_ref, v_ref, o_ref, own_ref, lse_ref, wo_ref, cos_ref, sin_ref, cosw_ref, sinw_ref, gg_ref, gu_ref,
                 dq_ref, dk_ref, dv_ref, go_ref, outg_ref, outu_ref, dh_s, do_s, dq_s, dk_s, dv_s, go_s, keep_s, send, recv, local, *, scale, bk):
    t = pl.program_id(0)
    place = Place(own_ref.shape[0])
    bq, width = q_ref.shape
    heads, half, wide = width // HEAD, outg_ref.shape[0], gg_ref.shape[1]
    seq, iq = turn_of(BACK)(t)
    e = scale * LOG2E
    g = Gather(place, dh_s, send, recv)
    theirs, mine = (pl.ds(pl.multiple_of(p * half, half), half) for p in (1 - place.p, place.p))
    there = chunks(gg_ref.at[theirs], outg_ref, 0, place.p * wide, wide) + chunks(gu_ref.at[theirs], outu_ref, 0, place.p * wide, wide)
    z = Swap(place, send, recv, N_MSG, there)
    cols = pl.ds(pl.multiple_of(place.p * wide, wide), wide)
    take = [pltpu.make_async_copy(a.at[mine], keep_s.at[n], local.at[n]) for n, a in enumerate((gg_ref, gu_ref))]
    put = [pltpu.make_async_copy(keep_s.at[n], a.at[:, cols], local.at[n]) for n, a in enumerate((outg_ref, outu_ref))]

    def begin():
        place.greet()
        dh_s[place.rows(0, 0), :] = own_ref[...]
        g.start()
        z.go("0")
        for copy in take:
            copy.start()
        go_s[...] = jnp.zeros_like(go_s)
        g.come("3")

    def first():
        g.middle()
        for a, b in zip(take, put):
            a.wait()
            b.start()
        g.come("a")

    def on(n):
        return lambda: z.go(n)

    happen(t, "-", {"0-": begin, "1-": serial(first, on("1")), "2-": serial(g.near, on("2"), come(g, "8")), "3-": serial(g.late, on("3"), come(g, "f")),
                    "4-": serial(g.last, on("4"), come(g, "6")), "5-": serial(on("5"), come(g, "e")), "6-": serial(on("6"), come(g, "c")),
                    "7-": serial(on("7"), come(g, "g"))})

    @pl.when(lax.rem(t, 4) == 0)
    def _():
        dk_s[...] = jnp.zeros_like(dk_s)
        dv_s[...] = jnp.zeros_like(dv_s)

    dh = dh_s[pl.ds(pl.multiple_of((seq * 4 + iq) * bq, bq), bq), :]
    dq_s[...] = jnp.zeros_like(dq_s)
    do_s[...] = nt(dh, wo_ref[...]).astype(BF16)
    go_s[...] += nn(o_ref[...].T, dh)
    parts = [slice(n * HEAD, (n + 1) * HEAD) for n in range(heads)]
    lses, deltas = [], []
    for n, c in enumerate(parts):
        lses.append(lse_ref[n : n + 1, :] * LOG2E)
        deltas.append((do_s[:, c].astype(F32) * o_ref[:, c].astype(F32)).T.sum(axis=0, keepdims=True))

    def tile(first, keys, q0, masked):
        here = pl.ds(pl.multiple_of(first, keys), keys)
        scores = [nt(k_ref[here, c], q_ref[q0:, c]) for c in parts]
        dps = [nt(v_ref[here, c], do_s[q0:, c]) for c in parts]
        if masked:
            shape = (keys, bq - q0)
            ok = lax.broadcasted_iota(jnp.int32, shape, 1) >= lax.broadcasted_iota(jnp.int32, shape, 0)
        for n, c in enumerate(parts):
            p = jnp.exp2(scores[n] * e - lses[n][:, q0:])
            if masked:
                p = jnp.where(ok, p, 0.0)
            ds = (p * (dps[n] - deltas[n][:, q0:])).astype(BF16)
            dv_s[n, here, :] += nn(p.astype(BF16), do_s[q0:, c])
            dk_s[n, here, :] += nn(ds, q_ref[q0:, c])
            dq_s[n, :, q0:] += nn(k_ref[here, c].T, ds)

    lax.fori_loop(0, iq, lambda j, _: tile(j * bq, bq, 0, False), None)
    for q0 in range(0, bq, bk):
        tile(iq * bq + q0, bk, q0, True)

    def back(a, cos, sin):
        a = a * scale
        return (a * cos - pltpu.roll(a, HEAD // 2, 1) * sin).astype(BF16)

    for n, c in enumerate(parts):
        dq_ref[:, c] = back(dq_s[n].T, cos_ref[...], sin_ref[...])

    @pl.when(lax.rem(t, 4) == 3)
    def _():
        for n, c in enumerate(parts):
            dk_ref[:, c] = back(dk_s[n], cosw_ref[...], sinw_ref[...])
            dv_ref[:, c] = dv_s[n].astype(BF16)

    @pl.when(t == pl.num_programs(0) - 1)
    def _():
        go_ref[...] = go_s[...].astype(BF16)
        for copy in put:
            copy.wait()
        z.come("01234567")
        g.sent()
        z.sent()


def attend_back(qkvs, o, own, lse, wo, cos, sin, gg, gu, n, bk=256):
    _, seqs, tokens, cols = qkvs.shape
    piece, d = own.shape
    bq, heads, half, wide = 2 * piece, cols // HEAD, gg.shape[0] // 2, gg.shape[1]
    at = lambda t: turn_of(BACK)(t)
    block = pl.BlockSpec((None, bq, cols), lambda t: (*at(t), 0))
    every = pl.BlockSpec((None, tokens, cols), lambda t: (at(t)[0], 0, 0))
    table = pl.BlockSpec((bq, HEAD), lambda t: (at(t)[1], 0))
    return pl.pallas_call(
        functools.partial(_attend_back, scale=HEAD**-0.5, bk=bk),
        grid=(len(BACK),),
        in_specs=[*three(at, tokens, bq, cols), block, whole(piece, d),
                  pl.BlockSpec((None, heads, bq), lambda t: (at(t)[0], 0, at(t)[1])), whole(cols, d), table, table, whole(tokens, HEAD), whole(tokens, HEAD), ANY, ANY],
        out_specs=[block, every, every, whole(cols, d), ANY, ANY],
        out_shape=[jax.ShapeDtypeStruct((seqs, tokens, cols), BF16)] * 3 + [jax.ShapeDtypeStruct((cols, d), BF16)] +
                  [jax.ShapeDtypeStruct((half, 2 * wide), BF16)] * 2,
        scratch_shapes=[pltpu.VMEM((seqs * tokens, d), BF16), pltpu.VMEM((bq, cols), BF16), pltpu.VMEM((heads, HEAD, bq), F32), pltpu.VMEM((heads, tokens, HEAD), F32),
                        pltpu.VMEM((heads, tokens, HEAD), F32), pltpu.VMEM((cols, d), F32), pltpu.VMEM((2, half, wide), BF16)] + sems(N_MSG + 8) +
                       [pltpu.SemaphoreType.DMA((2,))],
        compiler_params=comm_params(n), name="attend_back",
        cost_estimate=pl.CostEstimate(flops=10 * seqs * tokens * tokens * cols, transcendentals=0, bytes_accessed=16 * seqs * tokens * cols),
    )(qkvs, qkvs, qkvs, o, own, lse, wo, cos, sin, cos, sin, gg, gu)


LAST = kinds("1606141204021000")


def _qkv_back(x_ref, dh_ref, w_ref, at_ref, dq_ref, dk_ref, dv_ref, dx_ref, gq_ref, gk_ref, gv_ref,
              at_s, g_s, sum_s, low_s, da_s, peer, out, diag, block, across, send, recv, local, given, more):
    place = Place(x_ref.shape[0])
    both, half, cols, tokens = 2 * place.piece, gq_ref.shape[0], sum_s.shape[1], at_s.shape[1]
    s = Sum(place, da_s, peer, out, diag, block, across, send, recv)
    theirs, mine = (pl.ds(pl.multiple_of(p * half, half), half) for p in (1 - place.p, place.p))
    at = pl.ds(pl.multiple_of(place.p * cols, cols), cols)
    outs = (gq_ref, gk_ref, gv_ref)
    z = Swap(place, send, recv, N_MSG, [(low_s.at[n, theirs], o.at[:, at]) for n, o in enumerate(outs)])
    keep = [pltpu.make_async_copy(low_s.at[n, mine], o.at[:, at], local.at[n]) for n, o in enumerate(outs)]
    deep = tokens // 4
    parts = [pl.ds(c * deep, deep) for c in range(4)]
    loads = [pltpu.make_async_copy(at_ref.at[:, c], at_s.at[:, c], given.at[2 * n]) for n, c in enumerate(parts)]
    loadq = [pltpu.make_async_copy(dq_ref.at[c], g_s.at[0, c], given.at[2 * n + 1]) for n, c in enumerate(parts)]
    loadkv = [pltpu.make_async_copy(o, g_s.at[n + 1], more.at[n]) for n, o in enumerate((dk_ref, dv_ref))]
    for pair in zip(loads, loadq):
        for copy in pair:
            copy.start()
    for copy in loadkv:
        copy.start()
    place.greet()

    def give(m):
        low_s[m] = sum_s[...].astype(BF16)
        z.go(str(m))
        keep[m].start()

    def whole_of(m):
        sum_s[...] = jnp.zeros_like(sum_s)

        def go(n, _):
            here = pl.ds(pl.multiple_of(n * deep, deep), deep)
            sum_s[...] += nn(at_s[:, here], g_s[m, here, :])

        lax.fori_loop(0, 4, go, None)
        give(m)

    sum_s[...] = jnp.zeros_like(sum_s)

    def early(n, _):
        here = pl.ds(pl.multiple_of(n * deep, deep), deep)
        pltpu.make_async_copy(at_ref.at[:, here], at_s.at[:, here], given.at[2 * n]).wait()
        pltpu.make_async_copy(dq_ref.at[here], g_s.at[0, here], given.at[2 * n + 1]).wait()
        sum_s[...] += nn(at_s[:, here], g_s[0, here, :])

    lax.fori_loop(0, len(parts), early, None)
    give(0)
    for copy in loadkv:
        copy.wait()

    def step(n, _):
        seq, chip = turn_of(LAST)(n)
        rows = pl.ds(pl.multiple_of((seq * 4 + chip) * both, both), both)
        da_s[rows, :] = (nt(g_s[0, rows, :], w_ref[0]) + nt(g_s[1, rows, :], w_ref[1]) + nt(g_s[2, rows, :], w_ref[2])).astype(BF16)
        for k, kind in enumerate(LAST):
            pl.when(n == k)(functools.partial(s.start, *kind))
        happen(n, "-", {at: calls(s.deal, kind) for at, kind in zip("2367", LAST)})

    whole_of(1)
    lax.fori_loop(0, len(LAST), step, None)
    whole_of(2)
    for kind in kinds("04021000"):
        total = s.deal(*kind)
    dx_ref[...] = (dh_ref[...].astype(F32) + norm_back(x_ref[...], total)).astype(BF16)
    for copy in keep:
        copy.wait()
    z.come("012")
    z.sent()
    s.sent()


def qkv_back(at, dq, dk, dv, w, x, dh, n):
    piece, d = x.shape
    tokens, cols = dq.shape
    return pl.pallas_call(
        _qkv_back,
        in_specs=[IN_VMEM] * 3 + [ANY] * 4,
        out_specs=[IN_VMEM] + [ANY] * 3,
        out_shape=[jax.ShapeDtypeStruct((piece, d), BF16)] + [jax.ShapeDtypeStruct((d // 2, 2 * cols), BF16)] * 3,
        scratch_shapes=[pltpu.VMEM((d, tokens), BF16), pltpu.VMEM((3, tokens, cols), BF16), pltpu.VMEM((d, cols), F32), pltpu.VMEM((3, d, cols), BF16),
                        pltpu.VMEM((tokens, d), BF16)] + sum_scratch(piece, d) + sems(N_MSG + 3) + [pltpu.SemaphoreType.DMA((n,)) for n in (3, 8, 2)],
        compiler_params=comm_params(n), name="qkv_back",
        cost_estimate=pl.CostEstimate(flops=12 * tokens * d * cols, transcendentals=0, bytes_accessed=8 * tokens * cols),
    )(x, dh, w, at, dq, dk, dv)


def _settle(*refs):
    n = len(refs) // 3
    ins, outs, held, sem = refs[:n], refs[n : 2 * n], refs[2 * n : 3 * n], refs[-1]
    take = [pltpu.make_async_copy(a, b, sem.at[k]) for k, (a, b) in enumerate(zip(ins, held))]
    put = [pltpu.make_async_copy(b, c, sem.at[k]) for k, (b, c) in enumerate(zip(held, outs))]
    for copy in take:
        copy.start()
    for a, b in zip(take, put):
        a.wait()
        b.start()
    for copy in put:
        copy.wait()


def settle(arrays):
    n = len(arrays)
    return pl.pallas_call(
        _settle,
        in_specs=[ANY] * n, out_specs=[ANY] * n, out_shape=[jax.ShapeDtypeStruct(a.shape, a.dtype) for a in arrays],
        scratch_shapes=[pltpu.VMEM(a.shape, a.dtype) for a in arrays] + [pltpu.SemaphoreType.DMA((n,))],
        compiler_params=pltpu.CompilerParams(vmem_limit_bytes=VMEM), name="settle")(*arrays)


def solution(mesh):
    def step(x, dy, wq, wk, wv, wo, wg, wu, wd):
        x, dy = x[0], dy[0]
        qkvs, at, w, got0, dys, hide, cos, sin = qkv(x, dy, wd, wq, wk, wv, wg, 8 * x.shape[0], 0)
        qkvs = qkvs.reshape(3, 2, -1, qkvs.shape[-1])
        o, lse, h, b, got1, got2 = attend(qkvs, wo, x, wg, wu, 1)
        dh, gg, gu, gd = units(b, h, dy, dys, hide, (wg, wu, got0, got1, got2), 2)
        dq, dk, dv, go, gg, gu = attend_back(qkvs, o, dh, lse, wo, cos, sin, gg, gu, 3)
        dq, dk, dv = (t.reshape(-1, t.shape[-1]) for t in (dq, dk, dv))
        dx, gq, gk, gv = qkv_back(at, dq, dk, dv, w, x, dh, 4)
        gd, gg, gu, go, gq, gk, gv, dx = settle([gd, gg, gu, go, gq, gk, gv, dx])
        return dx[None], gq, gk, gv, go, gg, gu, gd

    states, by_columns, by_rows = P("dp", "tp", None), P("dp", "tp"), P(("tp", "dp"), None)
    weights = (by_columns, by_columns, by_columns, by_rows, by_columns, by_columns, by_rows)
    return jax.shard_map(step, mesh=mesh, in_specs=(states, states, *weights), out_specs=(states, *weights), check_vma=False)
```
